32 devices in a mesh: mem: 2 (over x), col: 16 (over z, y, core).
Axes of the slice: x: 2, y: 2, z: 4, core: 2. Of those that a mesh axis runs over, the one named last changes fastest.
Arguments:
- state_a: bfloat16 [64, 1048576], P('mem', 'col'), may hold values from -12 to 12
- state_b: bfloat16 [64, 1048576], P('mem', 'col'), may hold values from -12 to 12
- obs_index: int32 [2, 8192, 16], P(None, ('col', 'mem')), may hold values from 0 to 127
- observation_count: int32 [2, 8192], P(None, ('col', 'mem')), may hold values from 1 to 16, as said below
- obs_value: float32 [2, 8192, 16], P(None, ('col', 'mem')), may hold values from -32 to 32
- obs_weight: float32 [2, 8192, 16], P(None, ('col', 'mem')), may hold values from 0.02 to 0.2
Outputs:
- analysis_a: bfloat16 [64, 1048576], P(None, ('col', 'mem'))
- analysis_b: bfloat16 [64, 1048576], P(None, ('col', 'mem'))
- transform: float32 [64, 64], replicated
The draws below stay inside these ranges and needn't reach their ends.
Inputs may be any that keep to these rules, and one draw needn't show every extreme that they name: Slot s of block b of group g is an observation when s < observation_count[g, b]; for each group, every aligned run of 256 blocks holds a block with all 16 slots live.
All inputs are finite; a program needn't handle non-finite values.
Results may differ from the reference program's by a relative error of at most 0.005.
Values may be sent and summed in bfloat16 or wider, within the bound.
A program may use at most 64 MiB of HBM per device.

```python
import math
import jax
import jax.numpy as jnp
from jax import lax

K = 64
OBS_BLK = 16
ITERS = 24
NCOL = 1048576
PIECE = 32768
BPD = 256
NBLK = 8192


def group_parts(key, salt):
    key = jax.random.fold_in(key, salt)
    subkeys = jax.random.split(key, 8)
    patterns = jax.random.normal(subkeys[0], (K, 3), jnp.float32)
    amplitudes = jnp.exp(jax.random.uniform(subkeys[1], (3, 16), jnp.float32, jnp.log(0.2), jnp.log(1.6)))
    coefficients = jax.random.normal(subkeys[2], (3, NCOL), jnp.float32)
    scales = jnp.exp(jax.random.uniform(subkeys[3], (K,), jnp.float32, jnp.log(0.5), jnp.log(2.0)))
    member_noise = 0.5 * jax.random.normal(subkeys[4], (K, NCOL), jnp.float32)
    truth_noise = 0.5 * jax.random.normal(subkeys[5], (NCOL,), jnp.float32)
    offsets = jax.random.uniform(subkeys[6], (3,), jnp.float32, 1.0, 2.0)
    sign_flip = jnp.where(jax.random.uniform(subkeys[7], (3,), jnp.float32) < 0.5, -1.0, 1.0)
    driving = jnp.repeat(amplitudes, NCOL // 16, axis=1) * coefficients
    truth_coef = jnp.mean(patterns, axis=0) + offsets * sign_flip
    return (patterns, driving, scales, member_noise, truth_noise, truth_coef)


def member_field(key, salt):
    patterns, driving, scales, member_noise, truth_noise, truth_coef = group_parts(key, salt)
    member_values = scales[:, None] * member_noise + jnp.dot(patterns, driving, precision=lax.Precision.HIGHEST)
    return jnp.clip(member_values, -12.0, 12.0).astype(jnp.bfloat16)


def index_table(key):
    return jax.random.randint(jax.random.fold_in(key, 41), (2, NBLK, OBS_BLK), 0, 128).astype(jnp.int32)


def draw_state_a(key, part):
    return member_field(key, 11)


def draw_state_b(key, part):
    return member_field(key, 23)


def draw_obs_index(key, part):
    return index_table(key)


def draw_obs_value(key, part):
    observation_lookup = index_table(key)
    picked = []
    for group, salt in enumerate((11, 23)):
        patterns, driving, scales, member_noise, truth_noise, truth_coef = group_parts(key, salt)
        truth_field = jnp.dot(truth_coef, driving, precision=lax.Precision.HIGHEST) + truth_noise
        truth_field = jnp.clip(truth_field, -12.0, 12.0)
        picked.append(jnp.take_along_axis(truth_field.reshape(NBLK, 128), observation_lookup[group], axis=1))
    error_key = jax.random.fold_in(key, 53)
    errors = jnp.clip(jax.random.normal(error_key, (2, NBLK, OBS_BLK), jnp.float32), -4.0, 4.0)
    return jnp.stack(picked) + 5.0 * errors


def draw_observation_count(key, part):
    key = jax.random.fold_in(key, 37)
    first, second = jax.random.split(key)
    segs = NBLK // BPD
    counts = jax.random.randint(first, (2, segs, BPD), 1, OBS_BLK + 1)
    where_full = jax.random.randint(second, (2, segs, 1), 0, BPD)
    position = lax.broadcasted_iota(jnp.int32, (2, segs, BPD), 2)
    counts = jnp.where(position == where_full, OBS_BLK, counts)
    return counts.reshape(2, NBLK).astype(jnp.int32)


def level_of(stream_key, shape, cuts, low, top_value):
    def one(axis_at, blocks):
        heights = jax.random.uniform(jax.random.fold_in(jax.random.fold_in(stream_key, 6), axis_at), (blocks,), jnp.float32, low / len(cuts), top_value / len(cuts))
        return jnp.repeat(jnp.exp(heights), shape[axis_at] // blocks).reshape((-1,) + (1,) * (len(shape) - axis_at - 1))

    loudness = one(*cuts[0])
    for cut in cuts[1:]:
        loudness = loudness * one(*cut)
    return loudness


def setup_inputs(seed: int = 0) -> dict:
    splits = jax.random.split(jax.random.key(seed), 7)
    return {
        "state_a": draw_state_a(jax.random.fold_in(splits[6], 71), 0),
        "state_b": draw_state_b(jax.random.fold_in(splits[6], 71), 0),
        "obs_index": draw_obs_index(jax.random.fold_in(splits[6], 71), 0),
        "observation_count": draw_observation_count(jax.random.fold_in(splits[6], 71), 0),
        "obs_value": draw_obs_value(jax.random.fold_in(splits[6], 71), 0),
        "obs_weight": jnp.clip(jnp.exp(math.log(0.2) - 2.3025851 * jax.random.uniform(splits[5], (2, NBLK, OBS_BLK), jnp.float32) ** level_of(splits[5], (2, NBLK, OBS_BLK), ((1, 32),), -0.2, 0.2)), 0.02, 0.2),
    }


def inverse_root(amat):
    scale = jnp.sqrt(jnp.sum(amat * amat))
    eye = jnp.eye(amat.shape[0], dtype=jnp.float32)

    def forward_step(step, carry):
        yn, zn = carry
        tm = 1.5 * eye - 0.5 * jnp.dot(zn, yn, precision=lax.Precision.HIGHEST)
        return (jnp.dot(yn, tm, precision=lax.Precision.HIGHEST), jnp.dot(tm, zn, precision=lax.Precision.HIGHEST))
    yn, zn = lax.fori_loop(0, ITERS, forward_step, (amat / scale, eye))
    return (zn, scale)

def make_transform(gram_product, cross, misfit, total):
    members = gram_product.shape[0]
    scl = (members - 1.0) / total
    gs = scl * gram_product
    bs = scl * cross
    qval = scl * misfit
    tval = jnp.trace(gs)
    rho = (1.0 + qval / (members - 1.0)) / (1.0 + tval / (members - 1.0))
    amat = (members - 1.0) / rho * jnp.eye(members, dtype=jnp.float32) + gs
    zn, scale = inverse_root(amat)
    pmat = jnp.dot(zn, zn, precision=lax.Precision.HIGHEST) / scale
    wbar = jnp.dot(pmat, bs, precision=lax.Precision.HIGHEST)
    return jnp.sqrt(members - 1.0) * zn / jnp.sqrt(scale) + wbar[:, None]

def reference(state_a, state_b, obs_index, observation_count, obs_value, obs_weight):
    segs = NCOL // PIECE
    states = (state_a, state_b)

    def accumulate(carry, seg):
        gram_product, cross, misfit, total = carry
        for group in range(2):
            cols = lax.dynamic_slice_in_dim(states[group], seg * PIECE, PIECE, 1)
            idx = lax.dynamic_slice_in_dim(obs_index[group], seg * BPD, BPD, 0)
            cnt = lax.dynamic_slice_in_dim(observation_count[group], seg * BPD, BPD, 0)
            val = lax.dynamic_slice_in_dim(obs_value[group], seg * BPD, BPD, 0)
            wgt = lax.dynamic_slice_in_dim(obs_weight[group], seg * BPD, BPD, 0)
            live = (lax.broadcasted_iota(jnp.int32, (BPD, OBS_BLK), 1) < cnt[:, None]).astype(jnp.float32)
            blocks = cols.reshape(K, BPD, 128)
            hx = jnp.take_along_axis(blocks, jnp.broadcast_to(idx[None], (K, BPD, OBS_BLK)), axis=2).astype(jnp.float32)
            hmean = lax.optimization_barrier(jnp.mean(hx, axis=0))
            anomaly_rows = hx - hmean[None]
            innov = val - hmean
            wt = live * wgt
            scaled_anomaly = anomaly_rows * wt[None]
            gram_product = gram_product + jnp.einsum('nix,fix->nf', scaled_anomaly, anomaly_rows, precision=lax.Precision.HIGHEST)
            cross = cross + jnp.einsum('kbs,bs->k', scaled_anomaly, innov, precision=lax.Precision.HIGHEST)
            misfit = misfit + jnp.sum(wt * innov * innov)
            total = total + jnp.sum(live)
        return ((gram_product, cross, misfit, total), None)
    init = (jnp.zeros((K, K), jnp.float32), jnp.zeros((K,), jnp.float32), jnp.zeros((), jnp.float32), jnp.zeros((), jnp.float32))
    (gram_product, cross, misfit, total), _ = lax.scan(accumulate, init, jnp.arange(segs, dtype=jnp.int32))
    transform = make_transform(gram_product, cross, misfit, total)
    wb = transform.astype(jnp.bfloat16)
    column_total = lax.optimization_barrier(jnp.sum(wb.astype(jnp.float32), axis=0))
    ones = jnp.ones((K,), jnp.bfloat16)

    def analyse(state):

        def one_seg(seg):
            cols = lax.dynamic_slice_in_dim(state, seg * PIECE, PIECE, 1)
            xmean = jnp.dot(ones, cols, preferred_element_type=jnp.float32) / K
            mixed = jnp.dot(wb.T, cols, preferred_element_type=jnp.float32)
            return (mixed + xmean[None, :] * (1.0 - column_total)[:, None]).astype(jnp.bfloat16)
        pieces = lax.map(one_seg, jnp.arange(segs, dtype=jnp.int32))
        return jnp.transpose(pieces, (1, 0, 2)).reshape(K, NCOL)
    return (analyse(state_a), analyse(state_b), transform)
```

```python
import functools

import jax
import jax.numpy as jnp
from jax import lax
from jax.experimental import pallas as pl
from jax.experimental.pallas import tpu as pltpu
from jax.sharding import PartitionSpec as P

ITERS = 24
LANES = 128
HIGH = lax.Precision.HIGHEST
MESH = pl.DeviceIdType.MESH
ROWS = 128
UNIT = 1024
LATE = 0.25
AHEAD = 0.0625
EARLY_UNITS = 2
LATE_UNITS = 2
FIRST = 3
TILE = 2048


def bits(n):
    return [1 << i for i in range(n.bit_length() - 1)]


def transform_of(gram, members):
    g = gram[:members, :members]
    cross = gram[members : members + 1, :members]
    misfit = gram[members : members + 1, members : members + 1]
    total = gram[members + 1 : members + 2, members + 1 : members + 2]
    rows = lax.broadcasted_iota(jnp.int32, (members, members), 0)
    cols = lax.broadcasted_iota(jnp.int32, (members, members), 1)
    eye = (rows == cols).astype(jnp.float32)

    def whole(x):
        return jnp.sum(jnp.sum(x, axis=1, keepdims=True), axis=0, keepdims=True)

    def parts(x):
        hi = x.astype(jnp.bfloat16)
        rest = x - hi.astype(jnp.float32)
        mid = rest.astype(jnp.bfloat16)
        low = (rest - mid.astype(jnp.float32)).astype(jnp.bfloat16)
        return hi, mid, low

    def dot(a, b):
        total = None
        for i in range(3):
            left = jnp.concatenate(a[: 3 - i], axis=0) if i < 2 else a[0]
            out = jnp.dot(left, b[i], preferred_element_type=jnp.float32)
            for j in reversed(range(3 - i)):
                block = out[j * members : (j + 1) * members]
                total = block if total is None else total + block
        return total

    dof = members - 1.0
    scl = dof / total
    gs = scl * g
    bs = scl * cross
    rho = (1.0 + scl * misfit / dof) / (1.0 + whole(gs * eye) / dof)
    amat = dof / rho * eye + gs
    scale = jnp.sqrt(whole(amat * amat))

    def step(_, carry):
        yn, zn = carry
        yp, zp = parts(yn), parts(zn)
        tp = parts(1.5 * eye - 0.5 * dot(zp, yp))
        return dot(yp, tp), dot(tp, zp)

    _, zn = lax.fori_loop(0, ITERS, step, (amat / scale, eye))
    zp = parts(zn)
    wbar = jnp.sum(dot(zp, zp) / scale * bs, axis=1, keepdims=True)
    return jnp.sqrt(dof) * zn / jnp.sqrt(scale) + wbar


def plan(piece):
    units = piece // UNIT
    late = max(1, round(units * LATE))
    step = EARLY_UNITS if (units - late) % EARLY_UNITS == 0 else 1
    early = units - late
    sizes = []
    while sum(sizes) < late:
        sizes.append(min(LATE_UNITS, late - sum(sizes)))
    ahead, count = 0, 0
    while count < len(sizes) and ahead + sizes[count] <= max(1, round(units * AHEAD)):
        ahead += sizes[count]
        count += 1
    return units, early, step, sizes, count


def exchange_kernel(
    nmem, ncol, sa, sb, idx_hbm, val_hbm, wgt_hbm, cnt_hbm, oa, ob, tr,
    idx, val, wgt, cnt, table_sem, stage, idx_f, val_f, wgt_f, idx_tx, idx_in, tx, hx, cur, got, lhs,
    own_sem, stage_sem, idx_s, idx_r, hx_s, hx_r, st_s, st_r, red_s, red_r,
):
    me = lax.axis_index("mem")
    col = lax.axis_index("col")
    mk = sa.shape[0]
    members = mk * nmem
    piece = sa.shape[1] // nmem
    nblk = idx.shape[2]
    units, early, step, late_sizes, ahead = plan(piece)
    late = units - early
    state, out = (sa, sb), (oa, ob)
    peers = [lax.rem(me + d, nmem) for d in range(1, nmem)]
    across = [{"mem": me ^ b} for b in bits(nmem)] + [{"col": col ^ b} for b in bits(ncol)]

    def cols_of(owner, unit, size):
        return pl.ds(pl.multiple_of(owner * piece + unit * UNIT, LANES), size * UNIT)

    my_rows = pl.ds(pl.multiple_of(me * mk, mk), mk)

    loads = []
    for d, p in enumerate(peers):
        for g in range(2):
            loads.append(
                pltpu.make_async_copy(
                    state[g].at[:, cols_of(p, early, late)], stage.at[d, g], stage_sem.at[d, g]
                )
            )
    own = []
    for g in range(2):
        own.append(
            pltpu.make_async_copy(
                state[g].at[:, cols_of(me, 0, units)], out[g].at[my_rows, :], own_sem.at[g]
            )
        )
    tables = []
    for n, (a, b) in enumerate(((idx_hbm, idx), (val_hbm, val), (wgt_hbm, wgt), (cnt_hbm, cnt))):
        tables.append(pltpu.make_async_copy(a, b, table_sem.at[n]))
    for c in tables + loads + own:
        c.start()

    barrier = pltpu.get_barrier_semaphore()
    for p in peers:
        pl.semaphore_signal(barrier, inc=1, device_id={"mem": p}, device_id_type=MESH)
    for b in bits(ncol):
        pl.semaphore_signal(barrier, inc=1, device_id={"col": col ^ b}, device_id_type=MESH)
    pl.semaphore_wait(barrier, len(peers) + len(bits(ncol)))

    def move(slot, unit, size, g, d):
        return pltpu.make_async_remote_copy(
            state[g].at[:, cols_of(peers[d], unit, size)],
            out[g].at[my_rows, pl.ds(pl.multiple_of(unit * UNIT, LANES), size * UNIT)],
            st_s.at[slot],
            st_r.at[slot],
            device_id={"mem": peers[d]},
            device_id_type=MESH,
        )

    each = [(g, d) for g in range(2) for d in range(nmem - 1)]
    chunks = early // step

    def early_moves(q):
        return [move(q * len(each) + n, q * step, step, g, d) for n, (g, d) in enumerate(each)]

    late_moves = []
    at = early
    for n, size in enumerate(late_sizes):
        slot = (chunks + n) * len(each)
        late_moves.append((at, size, [move(slot + k, at, size, g, d) for k, (g, d) in enumerate(each)]))
        at += size

    def start_early(q, _):
        for m in early_moves(q):
            m.start()
        return 0

    first = min(FIRST, chunks)
    start_early(0, 0)

    for c in tables:
        c.wait()
    slot_of = lax.broadcasted_iota(jnp.int32, (16, nblk), 0)
    diag = (
        lax.broadcasted_iota(jnp.int32, (8, LANES), 0)
        == lax.broadcasted_iota(jnp.int32, (8, LANES), 1) // 16
    )

    def flat(x):
        x = jnp.concatenate([x] * 8, axis=0).T.reshape(units, 8, LANES)
        return jnp.sum(jnp.where(diag[None], x, 0.0), axis=1)

    for g in range(2):
        rows = flat(idx[g].astype(jnp.float32)).astype(jnp.int32)
        idx_f[g] = rows
        idx_tx[g] = rows[early:]
    for g in range(2):
        live = slot_of < cnt[g : g + 1, :]
        wgt_f[g] = flat(jnp.where(live, wgt[g], 0.0))
        val_f[g] = flat(val[g])

    idx_copies = []
    for d, p in enumerate(peers):
        idx_copies.append(
            pltpu.make_async_remote_copy(
                idx_tx, idx_in.at[d], idx_s.at[d], idx_r.at[d], device_id={"mem": p}, device_id_type=MESH
            )
        )
        idx_copies[-1].start()
    lax.fori_loop(1, first, start_early, 0)

    def gather(s, index):
        rows = s.shape[0]
        lane = lax.broadcasted_iota(jnp.int32, (rows, LANES), 1) // 16
        s = s.astype(jnp.float32)
        index = jnp.broadcast_to(index, (rows, LANES))
        picked = None
        for j in range(8):
            here = jnp.take_along_axis(s[:, j * LANES : (j + 1) * LANES], index, axis=1)
            picked = here if picked is None else jnp.where(lane == j, here, picked)
        return picked

    def lanes_of(unit):
        return pl.ds(pl.multiple_of(unit * LANES, LANES), LANES)

    def unit_cols(unit):
        return pl.ds(pl.multiple_of(unit * UNIT, LANES), UNIT)

    for c in loads:
        c.wait()
    hx_copies = []
    for d, p in enumerate(peers):
        src = nmem - 2 - d
        idx_copies[src].wait()
        for g in range(2):

            def send_row(u, _):
                picked = gather(stage[d, g, :, unit_cols(u)], idx_in[src, g, pl.ds(u, 1), :])
                tx[d, g, :, lanes_of(u)] = picked.astype(jnp.bfloat16)
                return 0

            lax.fori_loop(0, late, send_row, 0)
        hx_copies.append(
            pltpu.make_async_remote_copy(
                tx.at[d], hx.at[me], hx_s.at[d], hx_r.at[d], device_id={"mem": p}, device_id_type=MESH
            )
        )
    for c in own:
        c.wait()
    for g in range(2):

        def own_row(u, _):
            picked = gather(out[g][my_rows, unit_cols(early + u)], idx_f[g, pl.ds(early + u, 1), :])
            hx[me, g, :, lanes_of(u)] = picked.astype(jnp.bfloat16)
            return 0

        lax.fori_loop(0, late, own_row, 0)
    for c in hx_copies:
        c.start()
    lax.fori_loop(first, chunks, start_early, 0)
    for _, _, ms in late_moves[:ahead]:
        for m in ms:
            m.start()

    def product(acc, x, value, weight):
        hmean = jnp.sum(x, axis=0, keepdims=True) / members
        rest = jnp.zeros((ROWS - members - 1, x.shape[1]), jnp.float32)
        aug = jnp.concatenate([x - hmean, value - hmean, rest], axis=0)
        return acc + lax.dot_general(
            aug * weight, aug, (((1,), (1,)), ((), ())), precision=HIGH,
            preferred_element_type=jnp.float32,
        )

    def early_sum(q, acc):
        for m in early_moves(q):
            m.wait_recv()
        xs, vs, ws = [], [], []
        for g in range(2):
            for k in range(step):
                u = q * step + k
                xs.append(gather(out[g][:, unit_cols(u)], idx_f[g, pl.ds(u, 1), :]))
                vs.append(val_f[g, pl.ds(u, 1), :])
                ws.append(wgt_f[g, pl.ds(u, 1), :])
        return product(acc, *(jnp.concatenate(t, axis=1) for t in (xs, vs, ws)))

    acc = lax.fori_loop(0, chunks - 1, early_sum, jnp.zeros((ROWS, ROWS), jnp.float32))
    for c in hx_copies:
        c.wait()

    def late_sum(u, acc):
        x, value, weight = [], [], []
        for g in range(2):
            x.append(
                jnp.concatenate([hx[m, g, :, lanes_of(u)].astype(jnp.float32) for m in range(nmem)], axis=0)
            )
            value.append(val_f[g, pl.ds(early + u, 1), :])
            weight.append(wgt_f[g, pl.ds(early + u, 1), :])
        return product(acc, *(jnp.concatenate(t, axis=1) for t in (x, value, weight)))

    acc = lax.fori_loop(0, late, late_sum, acc)
    acc = early_sum(chunks - 1, acc)

    live = cnt[...].astype(jnp.float32)
    live = jnp.sum(jnp.sum(live, axis=1, keepdims=True), axis=0, keepdims=True)
    used = cur.shape[1]
    rows = lax.broadcasted_iota(jnp.int32, (used, LANES), 0)
    cols = lax.broadcasted_iota(jnp.int32, (used, LANES), 1)
    cur[0] = jnp.where((rows == members + 1) & (cols == members + 1), live, acc[:used])
    started = ahead
    for s, peer in enumerate(across):
        copy = pltpu.make_async_remote_copy(
            cur.at[s], got.at[s], red_s.at[s], red_r.at[s], device_id=peer, device_id_type=MESH
        )
        copy.start()
        if s + 1 == len(bits(nmem)):
            for _, _, ms in late_moves[started:]:
                for m in ms:
                    m.start()
        copy.wait()
        cur[s + 1] = cur[s] + got[s]
    if not bits(nmem):
        for _, _, ms in late_moves[started:]:
            for m in ms:
                m.start()
    weights = transform_of(cur[len(across)], members)
    tr[...] = weights
    wt = weights.T.astype(jnp.bfloat16)
    lhs[:members, :] = wt
    lhs[members:, :] = jnp.full((16, members), 1.0 / members, jnp.bfloat16)
    coef = 1.0 - jnp.sum(wt.astype(jnp.float32), axis=1, keepdims=True)

    def mix(at, size):
        where = pl.ds(pl.multiple_of(at, LANES), size)
        for g in range(2):
            mixed = jnp.dot(lhs[...], out[g][:, where], preferred_element_type=jnp.float32)
            xmean = mixed[members : members + 1]
            out[g][:, where] = (mixed[:members] + coef * xmean).astype(jnp.bfloat16)

    tile = TILE if (early * UNIT) % TILE == 0 else UNIT

    def mix_early(i, _):
        mix(i * tile, tile)
        return 0

    lax.fori_loop(0, early * UNIT // tile, mix_early, 0)
    for at, size, ms in late_moves:
        for m in ms:
            m.wait_recv()
        mix(at * UNIT, size * UNIT)

    def end_early(q, _):
        for m in early_moves(q):
            m.wait_send()
        return 0

    lax.fori_loop(0, chunks, end_early, 0)
    for _, _, ms in late_moves:
        for m in ms:
            m.wait_send()


def exchange(state_a, state_b, idx, val, wgt, cnt):
    nmem, ncol = lax.axis_size("mem"), lax.axis_size("col")
    mk, held = state_a.shape
    piece = held // nmem
    members = mk * nmem
    units, early, step, late_sizes, ahead = plan(piece)
    late = units - early
    steps = len(bits(nmem)) + len(bits(ncol))
    moves = 2 * (nmem - 1) * (early // step + len(late_sizes))
    used = (members + 2 + 7) // 8 * 8
    dma = pltpu.SemaphoreType.DMA
    hbm = pl.BlockSpec(memory_space=pltpu.HBM)
    vmem = pl.BlockSpec(memory_space=pltpu.VMEM)
    return pl.pallas_call(
        functools.partial(exchange_kernel, nmem, ncol),
        out_shape=(
            pltpu.VMEM((members, piece), jnp.bfloat16),
            pltpu.VMEM((members, piece), jnp.bfloat16),
            pltpu.VMEM((members, members), jnp.float32),
        ),
        in_specs=[hbm] * 6,
        out_specs=(vmem, vmem, vmem),
        scratch_shapes=[
            *(pltpu.VMEM(x.shape, x.dtype) for x in (idx, val, wgt, cnt)),
            dma((4,)),
            pltpu.VMEM((nmem - 1, 2, mk, late * UNIT), jnp.bfloat16),
            pltpu.VMEM((2, units, LANES), jnp.int32),
            pltpu.VMEM((2, units, LANES), jnp.float32),
            pltpu.VMEM((2, units, LANES), jnp.float32),
            pltpu.VMEM((2, late, LANES), jnp.int32),
            pltpu.VMEM((nmem - 1, 2, late, LANES), jnp.int32),
            pltpu.VMEM((nmem - 1, 2, mk, late * LANES), jnp.bfloat16),
            pltpu.VMEM((nmem, 2, mk, late * LANES), jnp.bfloat16),
            pltpu.VMEM((steps + 1, used, LANES), jnp.float32),
            pltpu.VMEM((steps, used, LANES), jnp.float32),
            pltpu.VMEM((members + 16, members), jnp.bfloat16),
            dma((2,)),
            dma((nmem - 1, 2)),
            dma((nmem - 1,)),
            dma((nmem - 1,)),
            dma((nmem - 1,)),
            dma((nmem - 1,)),
            dma((moves,)),
            dma((moves,)),
            dma((steps,)),
            dma((steps,)),
        ],
        compiler_params=pltpu.CompilerParams(
            collective_id=0, has_side_effects=True, vmem_limit_bytes=40 * 2**20
        ),
        name="exchange",
    )(*(pltpu.with_memory_space_constraint(x, pltpu.HBM) for x in (state_a, state_b, idx, val, wgt, cnt)))


def write_kernel(parts, xa, xb, tr, oa, ob, ot, sems, tr_sem):
    width = xa.shape[1] // parts
    copies = [pltpu.make_async_copy(tr, ot, tr_sem)]
    for i in range(parts):
        for g, (x, o) in enumerate(((xa, oa), (xb, ob))):
            where = pl.ds(i * width, width)
            copies.append(pltpu.make_async_copy(x.at[:, where], o.at[:, where], sems.at[g, i]))
    for c in copies:
        c.start()
    for c in copies:
        c.wait()


def write(xa, xb, tr):
    parts = 4
    vmem = pl.BlockSpec(memory_space=pltpu.VMEM)
    hbm = pl.BlockSpec(memory_space=pltpu.HBM)
    return pl.pallas_call(
        functools.partial(write_kernel, parts),
        out_shape=tuple(jax.ShapeDtypeStruct(x.shape, x.dtype) for x in (xa, xb, tr)),
        in_specs=[vmem, vmem, vmem],
        out_specs=(hbm, hbm, hbm),
        scratch_shapes=[pltpu.SemaphoreType.DMA((2, parts)), pltpu.SemaphoreType.DMA],
        compiler_params=pltpu.CompilerParams(vmem_limit_bytes=40 * 2**20),
        name="write",
    )(xa, xb, tr)


def shards(state_a, state_b, obs_index, observation_count, obs_value, obs_weight):
    tables = [jnp.transpose(x, (0, 2, 1)) for x in (obs_index, obs_value, obs_weight)]
    return write(*exchange(state_a, state_b, *tables, observation_count))


def solution(mesh):
    return jax.shard_map(
        shards,
        mesh=mesh,
        in_specs=(
            P("mem", "col"),
            P("mem", "col"),
            P(None, ("col", "mem"), None),
            P(None, ("col", "mem")),
            P(None, ("col", "mem"), None),
            P(None, ("col", "mem"), None),
        ),
        out_specs=(P(None, ("col", "mem")), P(None, ("col", "mem")), P()),
        check_vma=False,
    )
```

```python
import functools

import jax
import jax.numpy as jnp
from jax import lax
from jax.experimental import pallas as pl
from jax.experimental.pallas import tpu as pltpu
from jax.sharding import PartitionSpec as P

ITERS = 24
LANES = 128
HIGH = lax.Precision.HIGHEST
MESH = pl.DeviceIdType.MESH
ROWS = 128
UNIT = 1024
LATE = 0.3125
STEP = 2
FIRST = 3
TILE = 2048


def bits(n):
    return [1 << i for i in range(n.bit_length() - 1)]


def transform_of(gram, members):
    g = gram[:members, :members]
    cross = gram[members : members + 1, :members]
    misfit = gram[members : members + 1, members : members + 1]
    total = gram[members + 1 : members + 2, members + 1 : members + 2]
    rows = lax.broadcasted_iota(jnp.int32, (members, members), 0)
    cols = lax.broadcasted_iota(jnp.int32, (members, members), 1)
    eye = (rows == cols).astype(jnp.float32)

    def whole(x):
        return jnp.sum(jnp.sum(x, axis=1, keepdims=True), axis=0, keepdims=True)

    def parts(x):
        hi = x.astype(jnp.bfloat16)
        rest = x - hi.astype(jnp.float32)
        mid = rest.astype(jnp.bfloat16)
        low = (rest - mid.astype(jnp.float32)).astype(jnp.bfloat16)
        return hi, mid, low

    def dot(a, b):
        total = None
        for i in range(3):
            left = jnp.concatenate(a[: 3 - i], axis=0) if i < 2 else a[0]
            out = jnp.dot(left, b[i], preferred_element_type=jnp.float32)
            for j in reversed(range(3 - i)):
                block = out[j * members : (j + 1) * members]
                total = block if total is None else total + block
        return total

    dof = members - 1.0
    scl = dof / total
    gs = scl * g
    bs = scl * cross
    rho = (1.0 + scl * misfit / dof) / (1.0 + whole(gs * eye) / dof)
    amat = dof / rho * eye + gs
    scale = jnp.sqrt(whole(amat * amat))

    def step(_, carry):
        yn, zn = carry
        yp, zp = parts(yn), parts(zn)
        tp = parts(1.5 * eye - 0.5 * dot(zp, yp))
        return dot(yp, tp), dot(tp, zp)

    _, zn = lax.fori_loop(0, ITERS, step, (amat / scale, eye))
    zp = parts(zn)
    wbar = jnp.sum(dot(zp, zp) / scale * bs, axis=1, keepdims=True)
    return jnp.sqrt(dof) * zn / jnp.sqrt(scale) + wbar


def plan(piece):
    units = piece // UNIT
    step = STEP if units % STEP == 0 else 1
    late = max(1, round(units // step * LATE))
    return units, step, units // step - late, late


def sum_rounds(nmem, ncol):
    aside = 4 if ncol > 4 else 0
    gens = [(b, aside) for b in bits(nmem)] + [(0, b) for b in bits(ncol) if b > 1]
    rounds = []
    for i in range(0, len(gens), 2):
        pair = gens[i : i + 2]
        if len(pair) == 2:
            pair.append((pair[0][0] ^ pair[1][0], pair[0][1] ^ pair[1][1]))
        rounds.append(pair)
    return rounds


def exchange_kernel(
    nmem, ncol, sa, sb, idx_hbm, val_hbm, wgt_hbm, cnt_hbm, oa, ob, tr,
    idx, val, wgt, cnt, table_sem, stage, idx_f, val_f, wgt_f, idx_tx, idx_in, tx, hx, cur, got, res, lhs,
    own_sem, stage_sem, idx_s, idx_r, hx_s, hx_r, st_s, st_r, red_s, red_r, pair_s, pair_r, known,
):
    me = lax.axis_index("mem")
    col = lax.axis_index("col")
    mk = sa.shape[0]
    members = mk * nmem
    piece = sa.shape[1] // nmem
    nblk = idx.shape[2]
    units, step, chunks, late_chunks = plan(piece)
    early = chunks * step
    late = units - early
    state, out = (sa, sb), (oa, ob)
    peers = [lax.rem(me + d, nmem) for d in range(1, nmem)]
    rounds = sum_rounds(nmem, ncol)
    greeted = sorted({p for r in rounds for p in r if p[1]})
    paired = ncol > 1
    mate = {"col": col ^ 1}
    hub = lax.rem(col, 2) == 0

    def partner(p):
        return {"mem": me ^ p[0], "col": col ^ p[1]}

    def cols_of(owner, unit, size):
        return pl.ds(pl.multiple_of(owner * piece + unit * UNIT, LANES), size * UNIT)

    my_rows = pl.ds(pl.multiple_of(me * mk, mk), mk)

    loads = []
    for d, p in enumerate(peers):
        for g in range(2):
            loads.append(
                pltpu.make_async_copy(
                    state[g].at[:, cols_of(p, early, late)], stage.at[d, g], stage_sem.at[d, g]
                )
            )
    own = []
    for g in range(2):
        own.append(
            pltpu.make_async_copy(
                state[g].at[:, cols_of(me, 0, units)], out[g].at[my_rows, :], own_sem.at[g]
            )
        )
    tables = []
    for n, (a, b) in enumerate(((idx_hbm, idx), (val_hbm, val), (wgt_hbm, wgt), (cnt_hbm, cnt))):
        tables.append(pltpu.make_async_copy(a, b, table_sem.at[n]))
    for c in tables:
        c.start()

    barrier = pltpu.get_barrier_semaphore()
    for p in peers:
        pl.semaphore_signal(barrier, inc=1, device_id={"mem": p}, device_id_type=MESH)
    @pl.when(hub)
    def _():
        for p in greeted:
            pl.semaphore_signal(barrier, inc=1, device_id=partner(p), device_id_type=MESH)
        pl.semaphore_wait(barrier, len(peers) + len(greeted) + paired)
        if paired:
            pl.semaphore_signal(known, inc=1, device_id=mate, device_id_type=MESH)

    @pl.when(jnp.logical_not(hub))
    def _():
        pl.semaphore_signal(barrier, inc=1, device_id=mate, device_id_type=MESH)
        pl.semaphore_wait(barrier, len(peers))

    def move(slot, unit, size, g, d):
        return pltpu.make_async_remote_copy(
            state[g].at[:, cols_of(peers[d], unit, size)],
            out[g].at[my_rows, pl.ds(pl.multiple_of(unit * UNIT, LANES), size * UNIT)],
            st_s.at[slot],
            st_r.at[slot],
            device_id={"mem": peers[d]},
            device_id_type=MESH,
        )

    each = [(g, d) for g in range(2) for d in range(nmem - 1)]

    def moves(q):
        return [move(q * len(each) + n, q * step, step, g, d) for n, (g, d) in enumerate(each)]

    def start(q, _):
        for m in moves(q):
            m.start()
        return 0

    first = min(FIRST, chunks)
    start(0, 0)
    for c in loads + own:
        c.start()

    for c in tables:
        c.wait()
    slot_of = lax.broadcasted_iota(jnp.int32, (16, nblk), 0)
    diag = (
        lax.broadcasted_iota(jnp.int32, (8, LANES), 0)
        == lax.broadcasted_iota(jnp.int32, (8, LANES), 1) // 16
    )

    def flat(x):
        x = jnp.concatenate([x] * 8, axis=0).T.reshape(units, 8, LANES)
        return jnp.sum(jnp.where(diag[None], x, 0.0), axis=1)

    for g in range(2):
        rows = flat(idx[g].astype(jnp.float32)).astype(jnp.int32)
        idx_f[g] = rows
        idx_tx[g] = rows[early:]
    for g in range(2):
        live = slot_of < cnt[g : g + 1, :]
        wgt_f[g] = flat(jnp.where(live, wgt[g], 0.0))
        val_f[g] = flat(val[g])

    idx_copies = []
    for d, p in enumerate(peers):
        idx_copies.append(
            pltpu.make_async_remote_copy(
                idx_tx, idx_in.at[d], idx_s.at[d], idx_r.at[d], device_id={"mem": p}, device_id_type=MESH
            )
        )
        idx_copies[-1].start()
    lax.fori_loop(1, first, start, 0)

    def gather(s, index):
        rows = s.shape[0]
        lane = lax.broadcasted_iota(jnp.int32, (rows, LANES), 1) // 16
        s = s.astype(jnp.float32)
        index = jnp.broadcast_to(index, (rows, LANES))
        picked = None
        for j in range(8):
            here = jnp.take_along_axis(s[:, j * LANES : (j + 1) * LANES], index, axis=1)
            picked = here if picked is None else jnp.where(lane == j, here, picked)
        return picked

    def lanes_of(unit):
        return pl.ds(pl.multiple_of(unit * LANES, LANES), LANES)

    def unit_cols(unit):
        return pl.ds(pl.multiple_of(unit * UNIT, LANES), UNIT)

    for c in loads:
        c.wait()
    hx_copies = []
    for d, p in enumerate(peers):
        src = nmem - 2 - d
        idx_copies[src].wait()
        for g in range(2):

            def send_row(u, _):
                picked = gather(stage[d, g, :, unit_cols(u)], idx_in[src, g, pl.ds(u, 1), :])
                tx[d, g, :, lanes_of(u)] = picked.astype(jnp.bfloat16)
                return 0

            lax.fori_loop(0, late, send_row, 0)
        hx_copies.append(
            pltpu.make_async_remote_copy(
                tx.at[d], hx.at[me], hx_s.at[d], hx_r.at[d], device_id={"mem": p}, device_id_type=MESH
            )
        )
    for c in own:
        c.wait()
    for g in range(2):

        def own_row(u, _):
            picked = gather(out[g][my_rows, unit_cols(early + u)], idx_f[g, pl.ds(early + u, 1), :])
            hx[me, g, :, lanes_of(u)] = picked.astype(jnp.bfloat16)
            return 0

        lax.fori_loop(0, late, own_row, 0)
    for c in hx_copies:
        c.start()
    lax.fori_loop(first, chunks + late_chunks, start, 0)

    def product(acc, x, value, weight):
        hmean = jnp.sum(x, axis=0, keepdims=True) / members
        rest = jnp.zeros((ROWS - members - 1, x.shape[1]), jnp.float32)
        aug = jnp.concatenate([x - hmean, value - hmean, rest], axis=0)
        return acc + lax.dot_general(
            aug * weight, aug, (((1,), (1,)), ((), ())), precision=HIGH,
            preferred_element_type=jnp.float32,
        )

    def early_sum(q, acc):
        for m in moves(q):
            m.wait_recv()
        xs, vs, ws = [], [], []
        for g in range(2):
            for k in range(step):
                u = q * step + k
                xs.append(gather(out[g][:, unit_cols(u)], idx_f[g, pl.ds(u, 1), :]))
                vs.append(val_f[g, pl.ds(u, 1), :])
                ws.append(wgt_f[g, pl.ds(u, 1), :])
        return product(acc, *(jnp.concatenate(t, axis=1) for t in (xs, vs, ws)))

    acc = lax.fori_loop(0, chunks - 1, early_sum, jnp.zeros((ROWS, ROWS), jnp.float32))
    for c in hx_copies:
        c.wait()

    def late_sum(u, acc):
        x, value, weight = [], [], []
        for g in range(2):
            x.append(
                jnp.concatenate([hx[m, g, :, lanes_of(u)].astype(jnp.float32) for m in range(nmem)], axis=0)
            )
            value.append(val_f[g, pl.ds(early + u, 1), :])
            weight.append(wgt_f[g, pl.ds(early + u, 1), :])
        return product(acc, *(jnp.concatenate(t, axis=1) for t in (x, value, weight)))

    acc = lax.fori_loop(0, late, late_sum, acc)
    acc = early_sum(chunks - 1, acc)

    live = cnt[...].astype(jnp.float32)
    live = jnp.sum(jnp.sum(live, axis=1, keepdims=True), axis=0, keepdims=True)
    used = res.shape[0]
    rows = lax.broadcasted_iota(jnp.int32, (used, LANES), 0)
    cols = lax.broadcasted_iota(jnp.int32, (used, LANES), 1)
    acc = jnp.where((rows == members + 1) & (cols == members + 1), live, acc[:used])

    def to_mate(n, src, dst):
        return pltpu.make_async_remote_copy(
            src, dst, pair_s.at[n], pair_r.at[n], device_id=mate, device_id_type=MESH
        )

    @pl.when(hub)
    def _():
        total = acc
        if paired:
            to_mate(0, res, got.at[0]).wait_recv()
            total = total + got[0]
        slot = 1
        for n, r in enumerate(rounds):
            cur[n] = total
            copies = []
            for p in r:
                copies.append(
                    pltpu.make_async_remote_copy(
                        cur.at[n], got.at[slot + len(copies)],
                        red_s.at[slot + len(copies)], red_r.at[slot + len(copies)],
                        device_id=partner(p), device_id_type=MESH,
                    )
                )
            for c in copies:
                c.start()
            for c in copies:
                c.wait()
            total = total + got[slot]
            if len(r) == 3:
                total = total + (got[slot + 1] + got[slot + 2])
            slot += len(r)
        res[...] = total
        if paired:
            to_mate(1, res, res).start()

    @pl.when(jnp.logical_not(hub))
    def _():
        cur[0] = acc
        pl.semaphore_wait(known, 1)
        send = to_mate(0, cur.at[0], got.at[0])
        send.start()
        send.wait_send()
        to_mate(1, res, res).wait_recv()

    weights = transform_of(res[...], members)
    tr[...] = weights
    wt = weights.T.astype(jnp.bfloat16)
    lhs[:members, :] = wt
    lhs[members:, :] = jnp.full((16, members), 1.0 / members, jnp.bfloat16)
    coef = 1.0 - jnp.sum(wt.astype(jnp.float32), axis=1, keepdims=True)

    def mix(at, size):
        where = pl.ds(pl.multiple_of(at, LANES), size)
        for g in range(2):
            mixed = jnp.dot(lhs[...], out[g][:, where], preferred_element_type=jnp.float32)
            xmean = mixed[members : members + 1]
            out[g][:, where] = (mixed[:members] + coef * xmean).astype(jnp.bfloat16)

    tile = TILE if (early * UNIT) % TILE == 0 else UNIT

    def mix_early(i, _):
        mix(i * tile, tile)
        return 0

    lax.fori_loop(0, early * UNIT // tile, mix_early, 0)

    def mix_late(q, _):
        for m in moves(q):
            m.wait_recv()
        mix(q * step * UNIT, step * UNIT)
        return 0

    lax.fori_loop(chunks, chunks + late_chunks, mix_late, 0)

    def end(q, _):
        for m in moves(q):
            m.wait_send()
        return 0

    lax.fori_loop(0, chunks + late_chunks, end, 0)

    @pl.when(hub)
    def _():
        if paired:
            to_mate(1, res, res).wait_send()


def exchange(state_a, state_b, idx, val, wgt, cnt):
    nmem, ncol = lax.axis_size("mem"), lax.axis_size("col")
    mk, held = state_a.shape
    piece = held // nmem
    members = mk * nmem
    units, step, chunks, late_chunks = plan(piece)
    late = late_chunks * step
    rounds = sum_rounds(nmem, ncol)
    slots = 1 + sum(len(r) for r in rounds)
    moves = 2 * (nmem - 1) * (chunks + late_chunks)
    used = (members + 2 + 7) // 8 * 8
    dma = pltpu.SemaphoreType.DMA
    hbm = pl.BlockSpec(memory_space=pltpu.HBM)
    vmem = pl.BlockSpec(memory_space=pltpu.VMEM)
    return pl.pallas_call(
        functools.partial(exchange_kernel, nmem, ncol),
        out_shape=(
            pltpu.VMEM((members, piece), jnp.bfloat16),
            pltpu.VMEM((members, piece), jnp.bfloat16),
            pltpu.VMEM((members, members), jnp.float32),
        ),
        in_specs=[hbm] * 6,
        out_specs=(vmem, vmem, vmem),
        scratch_shapes=[
            *(pltpu.VMEM(x.shape, x.dtype) for x in (idx, val, wgt, cnt)),
            dma((4,)),
            pltpu.VMEM((nmem - 1, 2, mk, late * UNIT), jnp.bfloat16),
            pltpu.VMEM((2, units, LANES), jnp.int32),
            pltpu.VMEM((2, units, LANES), jnp.float32),
            pltpu.VMEM((2, units, LANES), jnp.float32),
            pltpu.VMEM((2, late, LANES), jnp.int32),
            pltpu.VMEM((nmem - 1, 2, late, LANES), jnp.int32),
            pltpu.VMEM((nmem - 1, 2, mk, late * LANES), jnp.bfloat16),
            pltpu.VMEM((nmem, 2, mk, late * LANES), jnp.bfloat16),
            pltpu.VMEM((max(1, len(rounds)), used, LANES), jnp.float32),
            pltpu.VMEM((slots, used, LANES), jnp.float32),
            pltpu.VMEM((used, LANES), jnp.float32),
            pltpu.VMEM((members + 16, members), jnp.bfloat16),
            dma((2,)),
            dma((nmem - 1, 2)),
            dma((nmem - 1,)),
            dma((nmem - 1,)),
            dma((nmem - 1,)),
            dma((nmem - 1,)),
            dma((moves,)),
            dma((moves,)),
            dma((slots,)),
            dma((slots,)),
            dma((2,)),
            dma((2,)),
            pltpu.SemaphoreType.REGULAR,
        ],
        compiler_params=pltpu.CompilerParams(
            collective_id=0, has_side_effects=True, vmem_limit_bytes=40 * 2**20
        ),
        name="exchange",
    )(*(pltpu.with_memory_space_constraint(x, pltpu.HBM) for x in (state_a, state_b, idx, val, wgt, cnt)))


def write_kernel(parts, xa, xb, tr, oa, ob, ot, sems, tr_sem):
    width = xa.shape[1] // parts
    copies = [pltpu.make_async_copy(tr, ot, tr_sem)]
    for i in range(parts):
        for g, (x, o) in enumerate(((xa, oa), (xb, ob))):
            where = pl.ds(i * width, width)
            copies.append(pltpu.make_async_copy(x.at[:, where], o.at[:, where], sems.at[g, i]))
    for c in copies:
        c.start()
    for c in copies:
        c.wait()


def write(xa, xb, tr):
    parts = 4
    vmem = pl.BlockSpec(memory_space=pltpu.VMEM)
    hbm = pl.BlockSpec(memory_space=pltpu.HBM)
    return pl.pallas_call(
        functools.partial(write_kernel, parts),
        out_shape=tuple(jax.ShapeDtypeStruct(x.shape, x.dtype) for x in (xa, xb, tr)),
        in_specs=[vmem, vmem, vmem],
        out_specs=(hbm, hbm, hbm),
        scratch_shapes=[pltpu.SemaphoreType.DMA((2, parts)), pltpu.SemaphoreType.DMA],
        compiler_params=pltpu.CompilerParams(vmem_limit_bytes=40 * 2**20),
        name="write",
    )(xa, xb, tr)


def shards(state_a, state_b, obs_index, observation_count, obs_value, obs_weight):
    tables = [jnp.transpose(x, (0, 2, 1)) for x in (obs_index, obs_value, obs_weight)]
    return write(*exchange(state_a, state_b, *tables, observation_count))


def solution(mesh):
    return jax.shard_map(
        shards,
        mesh=mesh,
        in_specs=(
            P("mem", "col"),
            P("mem", "col"),
            P(None, ("col", "mem"), None),
            P(None, ("col", "mem")),
            P(None, ("col", "mem"), None),
            P(None, ("col", "mem"), None),
        ),
        out_specs=(P(None, ("col", "mem")), P(None, ("col", "mem")), P()),
        check_vma=False,
    )
```

```python
import functools

import jax
import jax.numpy as jnp
from jax import lax
from jax.experimental import pallas as pl
from jax.experimental.pallas import tpu as pltpu
from jax.sharding import PartitionSpec as P

ITERS = 24
LANES = 128
HIGH = lax.Precision.HIGHEST
MESH = pl.DeviceIdType.MESH
ROWS = 128
UNIT = 1024
LATE = 0.3125
FIRST = 12
EARLY_SIZES = (1, 2, 4)
LATE_SIZES = (2, 4)
WIDE = 6144


def bits(n):
    return [1 << i for i in range(n.bit_length() - 1)]


def pack(sums, live, members):
    height = members * members // LANES
    rows = [sums[i : i + height, :members] for i in range(0, members, height)]
    lane = lax.broadcasted_iota(jnp.int32, (1, LANES), 1)
    last = jnp.where(lane == members + 1, live, sums[members : members + 1])
    return jnp.concatenate([jnp.concatenate(rows, axis=1), last, jnp.zeros((7, LANES), jnp.float32)], axis=0)


def transform_of(packed, members):
    height = members * members // LANES
    g = jnp.concatenate([packed[:height, i : i + members] for i in range(0, LANES, members)], axis=0)
    last = packed[height : height + 1]
    cross, misfit, total = last[:, :members], last[:, members : members + 1], last[:, members + 1 : members + 2]
    rows = lax.broadcasted_iota(jnp.int32, (members, members), 0)
    cols = lax.broadcasted_iota(jnp.int32, (members, members), 1)
    eye = (rows == cols).astype(jnp.float32)

    def whole(x):
        return jnp.sum(jnp.sum(x, axis=1, keepdims=True), axis=0, keepdims=True)

    def parts(x):
        hi = x.astype(jnp.bfloat16)
        rest = x - hi.astype(jnp.float32)
        mid = rest.astype(jnp.bfloat16)
        low = (rest - mid.astype(jnp.float32)).astype(jnp.bfloat16)
        return hi, mid, low

    def dot(a, b):
        total = None
        for i in range(3):
            left = jnp.concatenate(a[: 3 - i], axis=0) if i < 2 else a[0]
            out = jnp.dot(left, b[i], preferred_element_type=jnp.float32)
            for j in reversed(range(3 - i)):
                block = out[j * members : (j + 1) * members]
                total = block if total is None else total + block
        return total

    dof = members - 1.0
    scl = dof / total
    gs = scl * g
    bs = scl * cross
    rho = (1.0 + scl * misfit / dof) / (1.0 + whole(gs * eye) / dof)
    amat = dof / rho * eye + gs
    scale = jnp.sqrt(whole(amat * amat))

    def step(_, carry):
        yn, zn = carry
        yp, zp = parts(yn), parts(zn)
        tp = parts(1.5 * eye - 0.5 * dot(zp, yp))
        return dot(yp, tp), dot(tp, zp)

    _, zn = lax.fori_loop(0, ITERS, step, (amat / scale, eye))
    zp = parts(zn)
    wbar = jnp.sum(dot(zp, zp) / scale * bs, axis=1, keepdims=True)
    return jnp.sqrt(dof) * zn / jnp.sqrt(scale) + wbar


def cut(units, sizes):
    out = []
    while units:
        out.insert(0, min(units, sizes[min(len(out), len(sizes) - 1)]))
        units -= out[0]
    return out


def plan(piece):
    units = piece // UNIT
    late = max(1, round(units * LATE))
    at, moves = 0, []
    for part in cut(units - late, EARLY_SIZES), cut(late, LATE_SIZES):
        moves.append([])
        for n in part:
            moves[-1].append((at, n))
            at += n
    return units, *moves


def tiles(columns):
    n = 1
    while columns % (n * LANES) or columns // n > WIDE:
        n += 1
    return n, columns // n


def mixing(tr):
    members = tr.shape[0]
    wt = tr.T.astype(jnp.bfloat16)
    mean = jnp.full((16, members), 1.0 / members, jnp.bfloat16)
    return jnp.concatenate([wt, mean], axis=0), 1.0 - jnp.sum(wt.astype(jnp.float32), axis=1, keepdims=True)


def mix(lhs, coef, x):
    members = x.shape[0]
    mixed = jnp.dot(lhs, x, preferred_element_type=jnp.float32)
    return (mixed[:members] + coef * mixed[members : members + 1]).astype(x.dtype)


def sum_rounds(nmem, ncol):
    aside = 4 if ncol > 4 else 0
    gens = [(b, aside) for b in bits(nmem)] + [(0, b) for b in bits(ncol) if b > 1]
    rounds = []
    for i in range(0, len(gens), 2):
        pair = gens[i : i + 2]
        if len(pair) == 2:
            pair.append((pair[0][0] ^ pair[1][0], pair[0][1] ^ pair[1][1]))
        rounds.append(pair)
    return rounds


def exchange_kernel(
    nmem, ncol, sa, sb, idx_hbm, val_hbm, wgt_hbm, cnt_hbm, oa, ob, tr,
    idx, val, wgt, cnt, table_sem, stage, idx_f, val_f, wgt_f, idx_tx, idx_in, tx, hx, cur, got, res, lhs,
    own_sem, stage_sem, idx_s, idx_r, hx_s, hx_r, st_s, st_r, red_s, red_r, pair_s, pair_r, known,
):
    me = lax.axis_index("mem")
    col = lax.axis_index("col")
    mk = sa.shape[0]
    members = mk * nmem
    piece = sa.shape[1] // nmem
    nblk = idx.shape[2]
    units, early_moves, late_moves = plan(piece)
    early = late_moves[0][0]
    late = units - early
    state, out = (sa, sb), (oa, ob)
    peers = [lax.rem(me + d, nmem) for d in range(1, nmem)]
    rounds = sum_rounds(nmem, ncol)
    greeted = sorted({p for r in rounds for p in r if p[1]})
    paired = ncol > 1
    mate = {"col": col ^ 1}
    hub = lax.rem(col, 2) == 0

    def partner(p):
        return {"mem": me ^ p[0], "col": col ^ p[1]}

    def cols_of(owner, unit, size):
        return pl.ds(pl.multiple_of(owner * piece + unit * UNIT, LANES), size * UNIT)

    my_rows = pl.ds(pl.multiple_of(me * mk, mk), mk)

    loads = []
    for d, p in enumerate(peers):
        for g in range(2):
            loads.append(
                pltpu.make_async_copy(
                    state[g].at[:, cols_of(p, early, late)], stage.at[d, g], stage_sem.at[d, g]
                )
            )
    own = []
    for g in range(2):
        own.append(
            pltpu.make_async_copy(
                state[g].at[:, cols_of(me, 0, units)], out[g].at[my_rows, :], own_sem.at[g]
            )
        )
    tables = []
    for n, (a, b) in enumerate(((idx_hbm, idx), (val_hbm, val), (wgt_hbm, wgt), (cnt_hbm, cnt))):
        tables.append(pltpu.make_async_copy(a, b, table_sem.at[n]))
    for c in tables:
        c.start()

    barrier = pltpu.get_barrier_semaphore()
    for p in peers:
        pl.semaphore_signal(barrier, inc=1, device_id={"mem": p}, device_id_type=MESH)
    @pl.when(hub)
    def _():
        for p in greeted:
            pl.semaphore_signal(barrier, inc=1, device_id=partner(p), device_id_type=MESH)
        pl.semaphore_wait(barrier, len(peers) + len(greeted) + paired)
        if paired:
            pl.semaphore_signal(known, inc=1, device_id=mate, device_id_type=MESH)

    @pl.when(jnp.logical_not(hub))
    def _():
        pl.semaphore_signal(barrier, inc=1, device_id=mate, device_id_type=MESH)
        pl.semaphore_wait(barrier, len(peers))

    each = [(g, d) for g in range(2) for d in range(nmem - 1)]
    moves = []
    for at, size in early_moves + late_moves:
        moves.append([])
        for g, d in each:
            slot = (len(moves) - 1) * len(each) + len(moves[-1])
            moves[-1].append(
                pltpu.make_async_remote_copy(
                    state[g].at[:, cols_of(peers[d], at, size)],
                    out[g].at[my_rows, pl.ds(at * UNIT, size * UNIT)],
                    st_s.at[slot],
                    st_r.at[slot],
                    device_id={"mem": peers[d]},
                    device_id_type=MESH,
                )
            )
    first = len([at for at, _ in early_moves if 0 < at < FIRST]) + 1

    def start(some):
        for ms in some:
            for m in ms:
                m.start()

    start(moves[:1])
    for c in loads + own:
        c.start()

    for c in tables:
        c.wait()
    slot_of = lax.broadcasted_iota(jnp.int32, (16, nblk), 0)
    diag = (
        lax.broadcasted_iota(jnp.int32, (8, LANES), 0)
        == lax.broadcasted_iota(jnp.int32, (8, LANES), 1) // 16
    )

    def flat(x):
        x = jnp.concatenate([x] * 8, axis=0).T.reshape(units, 8, LANES)
        return jnp.sum(jnp.where(diag[None], x, 0.0), axis=1)

    for g in range(2):
        rows = flat(idx[g].astype(jnp.float32)).astype(jnp.int32)
        idx_f[g] = rows
        idx_tx[g] = rows[early:]
    for g in range(2):
        live = slot_of < cnt[g : g + 1, :]
        wgt_f[g] = flat(jnp.where(live, wgt[g], 0.0))
        val_f[g] = flat(val[g])

    idx_copies = []
    for d, p in enumerate(peers):
        idx_copies.append(
            pltpu.make_async_remote_copy(
                idx_tx, idx_in.at[d], idx_s.at[d], idx_r.at[d], device_id={"mem": p}, device_id_type=MESH
            )
        )
        idx_copies[-1].start()
    start(moves[1:first])

    def gather(s, index):
        rows = s.shape[0]
        lane = lax.broadcasted_iota(jnp.int32, (rows, LANES), 1) // 16
        s = s.astype(jnp.float32)
        index = jnp.broadcast_to(index, (rows, LANES))
        picked = None
        for j in range(8):
            here = jnp.take_along_axis(s[:, j * LANES : (j + 1) * LANES], index, axis=1)
            picked = here if picked is None else jnp.where(lane == j, here, picked)
        return picked

    def lanes_of(unit):
        return pl.ds(pl.multiple_of(unit * LANES, LANES), LANES)

    def unit_cols(unit):
        return pl.ds(pl.multiple_of(unit * UNIT, LANES), UNIT)

    for c in loads:
        c.wait()
    hx_copies = []
    for d, p in enumerate(peers):
        src = nmem - 2 - d
        idx_copies[src].wait()
        for g in range(2):

            def send_row(u, _):
                picked = gather(stage[d, g, :, unit_cols(u)], idx_in[src, g, pl.ds(u, 1), :])
                tx[d, g, :, lanes_of(u)] = picked.astype(jnp.bfloat16)
                return 0

            lax.fori_loop(0, late, send_row, 0)
        hx_copies.append(
            pltpu.make_async_remote_copy(
                tx.at[d], hx.at[me], hx_s.at[d], hx_r.at[d], device_id={"mem": p}, device_id_type=MESH
            )
        )
    for c in own:
        c.wait()
    for g in range(2):

        def own_row(u, _):
            picked = gather(out[g][my_rows, unit_cols(early + u)], idx_f[g, pl.ds(early + u, 1), :])
            hx[me, g, :, lanes_of(u)] = picked.astype(jnp.bfloat16)
            return 0

        lax.fori_loop(0, late, own_row, 0)
    for c in hx_copies:
        c.start()
    start(moves[first:])

    def product(acc, x, value, weight):
        hmean = jnp.sum(x, axis=0, keepdims=True) / members
        rest = jnp.zeros((ROWS - members - 1, x.shape[1]), jnp.float32)
        aug = jnp.concatenate([x - hmean, value - hmean, rest], axis=0)
        return acc + lax.dot_general(
            aug * weight, aug, (((1,), (1,)), ((), ())), precision=HIGH,
            preferred_element_type=jnp.float32,
        )

    def early_sum(u, acc):
        for n, (at, _) in enumerate(early_moves):

            @pl.when(u == at)
            def _():
                for m in moves[n]:
                    m.wait_recv()

        x = [gather(out[g][:, unit_cols(u)], idx_f[g, pl.ds(u, 1), :]) for g in range(2)]
        value = [val_f[g, pl.ds(u, 1), :] for g in range(2)]
        weight = [wgt_f[g, pl.ds(u, 1), :] for g in range(2)]
        return product(acc, *(jnp.concatenate(t, axis=1) for t in (x, value, weight)))

    acc = lax.fori_loop(0, early - 1, early_sum, jnp.zeros((ROWS, ROWS), jnp.float32))
    for c in hx_copies:
        c.wait()

    def late_sum(u, acc):
        x, value, weight = [], [], []
        for g in range(2):
            x.append(
                jnp.concatenate([hx[m, g, :, lanes_of(u)].astype(jnp.float32) for m in range(nmem)], axis=0)
            )
            value.append(val_f[g, pl.ds(early + u, 1), :])
            weight.append(wgt_f[g, pl.ds(early + u, 1), :])
        return product(acc, *(jnp.concatenate(t, axis=1) for t in (x, value, weight)))

    acc = lax.fori_loop(0, late, late_sum, acc)
    acc = early_sum(early - 1, acc)

    live = cnt[...].astype(jnp.float32)
    live = jnp.sum(jnp.sum(live, axis=1, keepdims=True), axis=0, keepdims=True)
    acc = pack(acc, live, members)

    def to_mate(n, src, dst):
        return pltpu.make_async_remote_copy(
            src, dst, pair_s.at[n], pair_r.at[n], device_id=mate, device_id_type=MESH
        )

    @pl.when(hub)
    def _():
        total = acc
        if paired:
            to_mate(0, res, got.at[0]).wait_recv()
            total = total + got[0]
        slot = 1
        for n, r in enumerate(rounds):
            cur[n] = total
            copies = []
            for p in r:
                copies.append(
                    pltpu.make_async_remote_copy(
                        cur.at[n], got.at[slot + len(copies)],
                        red_s.at[slot + len(copies)], red_r.at[slot + len(copies)],
                        device_id=partner(p), device_id_type=MESH,
                    )
                )
            for c in copies:
                c.start()
            for c in copies:
                c.wait()
            total = total + got[slot]
            if len(r) == 3:
                total = total + (got[slot + 1] + got[slot + 2])
            slot += len(r)
        res[...] = total
        if paired:
            to_mate(1, res, res).start()

    @pl.when(jnp.logical_not(hub))
    def _():
        cur[0] = acc
        pl.semaphore_wait(known, 1)
        send = to_mate(0, cur.at[0], got.at[0])
        send.start()
        send.wait_send()
        to_mate(1, res, res).wait_recv()

    weights = transform_of(res[...], members)
    tr[...] = weights
    left, coef = mixing(weights)
    lhs[...] = left
    count, width = tiles(early * UNIT)

    def mix_tile(i, _):
        where = pl.ds(pl.multiple_of(i * width, LANES), width)
        for g in range(2):
            out[g][:, where] = mix(lhs[...], coef, out[g][:, where])
        return 0

    lax.fori_loop(0, count, mix_tile, 0)
    for ms in moves[len(early_moves) :]:
        for m in ms:
            m.wait_recv()
    for ms in moves:
        for m in ms:
            m.wait_send()

    @pl.when(hub)
    def _():
        if paired:
            to_mate(1, res, res).wait_send()


def exchange(state_a, state_b, idx, val, wgt, cnt):
    nmem, ncol = lax.axis_size("mem"), lax.axis_size("col")
    mk, held = state_a.shape
    piece = held // nmem
    members = mk * nmem
    units, early_moves, late_moves = plan(piece)
    late = units - late_moves[0][0]
    rounds = sum_rounds(nmem, ncol)
    slots = 1 + sum(len(r) for r in rounds)
    moves = 2 * (nmem - 1) * len(early_moves + late_moves)
    used = members * members // LANES + 8
    dma = pltpu.SemaphoreType.DMA
    hbm = pl.BlockSpec(memory_space=pltpu.HBM)
    vmem = pl.BlockSpec(memory_space=pltpu.VMEM)
    return pl.pallas_call(
        functools.partial(exchange_kernel, nmem, ncol),
        out_shape=(
            pltpu.VMEM((members, piece), jnp.bfloat16),
            pltpu.VMEM((members, piece), jnp.bfloat16),
            pltpu.VMEM((members, members), jnp.float32),
        ),
        in_specs=[hbm] * 6,
        out_specs=(vmem, vmem, vmem),
        scratch_shapes=[
            *(pltpu.VMEM(x.shape, x.dtype) for x in (idx, val, wgt, cnt)),
            dma((4,)),
            pltpu.VMEM((nmem - 1, 2, mk, late * UNIT), jnp.bfloat16),
            pltpu.VMEM((2, units, LANES), jnp.int32),
            pltpu.VMEM((2, units, LANES), jnp.float32),
            pltpu.VMEM((2, units, LANES), jnp.float32),
            pltpu.VMEM((2, late, LANES), jnp.int32),
            pltpu.VMEM((nmem - 1, 2, late, LANES), jnp.int32),
            pltpu.VMEM((nmem - 1, 2, mk, late * LANES), jnp.bfloat16),
            pltpu.VMEM((nmem, 2, mk, late * LANES), jnp.bfloat16),
            pltpu.VMEM((max(1, len(rounds)), used, LANES), jnp.float32),
            pltpu.VMEM((slots, used, LANES), jnp.float32),
            pltpu.VMEM((used, LANES), jnp.float32),
            pltpu.VMEM((members + 16, members), jnp.bfloat16),
            dma((2,)),
            dma((nmem - 1, 2)),
            dma((nmem - 1,)),
            dma((nmem - 1,)),
            dma((nmem - 1,)),
            dma((nmem - 1,)),
            dma((moves,)),
            dma((moves,)),
            dma((slots,)),
            dma((slots,)),
            dma((2,)),
            dma((2,)),
            pltpu.SemaphoreType.REGULAR,
        ],
        compiler_params=pltpu.CompilerParams(
            collective_id=0, has_side_effects=True, vmem_limit_bytes=40 * 2**20
        ),
        name="exchange",
    )(*(pltpu.with_memory_space_constraint(x, pltpu.HBM) for x in (state_a, state_b, idx, val, wgt, cnt)))


def write_kernel(early, xa, xb, tr, oa, ob, ot, mixed, early_sem, late_sem, tr_sem):
    copies = [pltpu.make_async_copy(tr, ot, tr_sem)]
    count = early_sem.shape[1]
    for i in range(count):
        for g, (x, o) in enumerate(((xa, oa), (xb, ob))):
            where = pl.ds(i * (early // count), early // count)
            copies.append(pltpu.make_async_copy(x.at[:, where], o.at[:, where], early_sem.at[g, i]))
    for c in copies:
        c.start()
    lhs, coef = mixing(tr[...])
    width = mixed.shape[3]
    for i in range(mixed.shape[0]):
        for g, (x, o) in enumerate(((xa, oa), (xb, ob))):
            where = pl.ds(early + i * width, width)
            mixed[i, g] = mix(lhs, coef, x[:, where])
            copies.append(pltpu.make_async_copy(mixed.at[i, g], o.at[:, where], late_sem.at[g, i]))
            copies[-1].start()
    for c in copies:
        c.wait()


def write(xa, xb, tr):
    members, piece = xa.shape
    early = plan(piece)[2][0][0] * UNIT
    count, width = tiles(piece - early)
    parts = 2
    vmem = pl.BlockSpec(memory_space=pltpu.VMEM)
    hbm = pl.BlockSpec(memory_space=pltpu.HBM)
    dma = pltpu.SemaphoreType.DMA
    return pl.pallas_call(
        functools.partial(write_kernel, early),
        out_shape=tuple(jax.ShapeDtypeStruct(x.shape, x.dtype) for x in (xa, xb, tr)),
        in_specs=[vmem, vmem, vmem],
        out_specs=(hbm, hbm, hbm),
        scratch_shapes=[
            pltpu.VMEM((count, 2, members, width), xa.dtype),
            dma((2, parts)),
            dma((2, count)),
            dma,
        ],
        compiler_params=pltpu.CompilerParams(vmem_limit_bytes=40 * 2**20),
        name="write",
    )(xa, xb, tr)


def shards(state_a, state_b, obs_index, observation_count, obs_value, obs_weight):
    tables = [jnp.transpose(x, (0, 2, 1)) for x in (obs_index, obs_value, obs_weight)]
    return write(*exchange(state_a, state_b, *tables, observation_count))


def solution(mesh):
    return jax.shard_map(
        shards,
        mesh=mesh,
        in_specs=(
            P("mem", "col"),
            P("mem", "col"),
            P(None, ("col", "mem"), None),
            P(None, ("col", "mem")),
            P(None, ("col", "mem"), None),
            P(None, ("col", "mem"), None),
        ),
        out_specs=(P(None, ("col", "mem")), P(None, ("col", "mem")), P()),
        check_vma=False,
    )
```

```python
import functools

import jax
import jax.numpy as jnp
from jax import lax
from jax.experimental import pallas as pl
from jax.experimental.pallas import tpu as pltpu
from jax.sharding import PartitionSpec as P

ITERS = 24
LANES = 128
HIGH = lax.Precision.HIGHEST
MESH = pl.DeviceIdType.MESH
ROWS = 128
UNIT = 1024
LATE = 0.40625
FIRST = 12
EARLY_SIZES = (1, 2, 4)
LATE_SIZES = (2, 4)
REST = UNIT - LANES
WIDE = 6144


def bits(n):
    return [1 << i for i in range(n.bit_length() - 1)]


def pack(sums, live, members):
    height = members * members // LANES
    rows = [sums[i : i + height, :members] for i in range(0, members, height)]
    lane = lax.broadcasted_iota(jnp.int32, (1, LANES), 1)
    last = jnp.where(lane == members + 1, live, sums[members : members + 1])
    return jnp.concatenate([jnp.concatenate(rows, axis=1), last, jnp.zeros((7, LANES), jnp.float32)], axis=0)


def transform_of(packed, members):
    height = members * members // LANES
    g = jnp.concatenate([packed[:height, i : i + members] for i in range(0, LANES, members)], axis=0)
    last = packed[height : height + 1]
    cross, misfit, total = last[:, :members], last[:, members : members + 1], last[:, members + 1 : members + 2]
    rows = lax.broadcasted_iota(jnp.int32, (members, members), 0)
    cols = lax.broadcasted_iota(jnp.int32, (members, members), 1)
    eye = (rows == cols).astype(jnp.float32)

    def whole(x):
        return jnp.sum(jnp.sum(x, axis=1, keepdims=True), axis=0, keepdims=True)

    def parts(x):
        hi = x.astype(jnp.bfloat16)
        rest = x - hi.astype(jnp.float32)
        mid = rest.astype(jnp.bfloat16)
        low = (rest - mid.astype(jnp.float32)).astype(jnp.bfloat16)
        return hi, mid, low

    def dot(a, b):
        total = None
        for i in range(3):
            left = jnp.concatenate(a[: 3 - i], axis=0) if i < 2 else a[0]
            out = jnp.dot(left, b[i], preferred_element_type=jnp.float32)
            for j in reversed(range(3 - i)):
                block = out[j * members : (j + 1) * members]
                total = block if total is None else total + block
        return total

    dof = members - 1.0
    scl = dof / total
    gs = scl * g
    bs = scl * cross
    rho = (1.0 + scl * misfit / dof) / (1.0 + whole(gs * eye) / dof)
    amat = dof / rho * eye + gs
    scale = jnp.sqrt(whole(amat * amat))

    def step(_, carry):
        yn, zn = carry
        yp, zp = parts(yn), parts(zn)
        tp = parts(1.5 * eye - 0.5 * dot(zp, yp))
        return dot(yp, tp), dot(tp, zp)

    _, zn = lax.fori_loop(0, ITERS, step, (amat / scale, eye))
    zp = parts(zn)
    wbar = jnp.sum(dot(zp, zp) / scale * bs, axis=1, keepdims=True)
    return jnp.sqrt(dof) * zn / jnp.sqrt(scale) + wbar


def cut(units, sizes):
    out = []
    while units:
        out.insert(0, min(units, sizes[min(len(out), len(sizes) - 1)]))
        units -= out[0]
    return out


def plan(piece):
    units = piece // UNIT
    late = max(1, round(units * LATE))
    at, moves = 0, []
    for part in cut(units - late, EARLY_SIZES), cut(late, LATE_SIZES):
        moves.append([])
        for n in part:
            moves[-1].append((at, n))
            at += n
    return units, *moves


def tiles(columns):
    n = 1
    while columns % (n * LANES) or columns // n > WIDE:
        n += 1
    return n, columns // n


def mixing(tr):
    members = tr.shape[0]
    wt = tr.T.astype(jnp.bfloat16)
    mean = jnp.full((16, members), 1.0 / members, jnp.bfloat16)
    return jnp.concatenate([wt, mean], axis=0), 1.0 - jnp.sum(wt.astype(jnp.float32), axis=1, keepdims=True)


def mix(lhs, coef, x):
    members = x.shape[0]
    mixed = jnp.dot(lhs, x, preferred_element_type=jnp.float32)
    return (mixed[:members] + coef * mixed[members : members + 1]).astype(x.dtype)


def sum_rounds(nmem, ncol):
    aside = 4 if ncol > 4 else 0
    gens = [(b, aside) for b in bits(nmem)] + [(0, b) for b in bits(ncol) if b > 1]
    rounds = []
    for i in range(0, len(gens), 2):
        pair = gens[i : i + 2]
        if len(pair) == 2:
            pair.append((pair[0][0] ^ pair[1][0], pair[0][1] ^ pair[1][1]))
        rounds.append(pair)
    return rounds


def exchange_kernel(
    nmem, ncol, sa, sb, idx_hbm, val_hbm, wgt_hbm, cnt_hbm, oa, ob, tr,
    idx, val, wgt, cnt, table_sem, stage, idx_f, val_f, wgt_f, idx_tx, idx_in,
    from_s, from_c, at_s, back, tx, rest_tx, ahead_in, rest_in, hx, cur, got, res, lhs,
    own_sem, stage_sem, idx_s, idx_r, hx_s, hx_r, st_s, st_r, red_s, red_r, pair_s, pair_r, known,
):
    me = lax.axis_index("mem")
    col = lax.axis_index("col")
    mk = sa.shape[0]
    members = mk * nmem
    piece = sa.shape[1] // nmem
    nblk = idx.shape[2]
    units, early_moves, late_moves = plan(piece)
    early = late_moves[0][0]
    late = units - early
    state, out = (sa, sb), (oa, ob)
    peers = [lax.rem(me + d, nmem) for d in range(1, nmem)]
    rounds = sum_rounds(nmem, ncol)
    greeted = sorted({p for r in rounds for p in r if p[1]})
    paired = ncol > 1
    mate = {"col": col ^ 1}
    hub = lax.rem(col, 2) == 0

    def partner(p):
        return {"mem": me ^ p[0], "col": col ^ p[1]}

    def cols_of(owner, unit, size):
        return pl.ds(pl.multiple_of(owner * piece + unit * UNIT, LANES), size * UNIT)

    my_rows = pl.ds(pl.multiple_of(me * mk, mk), mk)

    loads = []
    for d, p in enumerate(peers):
        for g in range(2):
            loads.append(
                pltpu.make_async_copy(
                    state[g].at[:, cols_of(p, early, late)], stage.at[d, g], stage_sem.at[d, g]
                )
            )
    own = []
    for g in range(2):
        own.append(
            pltpu.make_async_copy(
                state[g].at[:, cols_of(me, 0, units)], out[g].at[my_rows, :], own_sem.at[g]
            )
        )
    tables = []
    for n, (a, b) in enumerate(((idx_hbm, idx), (val_hbm, val), (wgt_hbm, wgt), (cnt_hbm, cnt))):
        tables.append(pltpu.make_async_copy(a, b, table_sem.at[n]))
    for c in tables:
        c.start()

    barrier = pltpu.get_barrier_semaphore()
    for p in peers:
        pl.semaphore_signal(barrier, inc=1, device_id={"mem": p}, device_id_type=MESH)
    @pl.when(hub)
    def _():
        for p in greeted:
            pl.semaphore_signal(barrier, inc=1, device_id=partner(p), device_id_type=MESH)
        pl.semaphore_wait(barrier, len(peers) + len(greeted) + paired)
        if paired:
            pl.semaphore_signal(known, inc=1, device_id=mate, device_id_type=MESH)

    @pl.when(jnp.logical_not(hub))
    def _():
        pl.semaphore_signal(barrier, inc=1, device_id=mate, device_id_type=MESH)
        pl.semaphore_wait(barrier, len(peers))

    each = [(g, d) for g in range(2) for d in range(nmem - 1)]
    moves = []
    for at, size in early_moves + late_moves:
        moves.append([])
        for g, d in each:
            slot = (len(moves) - 1) * len(each) + len(moves[-1])
            if at < early:
                source = state[g].at[:, cols_of(peers[d], at, size)]
                target = out[g].at[my_rows, pl.ds(at * UNIT, size * UNIT)]
            else:
                where = pl.ds((at - early) * REST, size * REST)
                source, target = rest_tx.at[d, g, :, where], rest_in.at[me, g, :, where]
            moves[-1].append(
                pltpu.make_async_remote_copy(
                    source, target, st_s.at[slot], st_r.at[slot],
                    device_id={"mem": peers[d]}, device_id_type=MESH,
                )
            )
    first = len([at for at, _ in early_moves if 0 < at < FIRST]) + 1

    def start(some):
        for ms in some:
            for m in ms:
                m.start()

    start(moves[:1])
    for c in loads + own:
        c.start()

    for c in tables:
        c.wait()
    slot_of = lax.broadcasted_iota(jnp.int32, (16, nblk), 0)
    diag = (
        lax.broadcasted_iota(jnp.int32, (8, LANES), 0)
        == lax.broadcasted_iota(jnp.int32, (8, LANES), 1) // 16
    )

    def flat(x):
        x = jnp.concatenate([x] * 8, axis=0).T.reshape(units, 8, LANES)
        return jnp.sum(jnp.where(diag[None], x, 0.0), axis=1)

    for g in range(2):
        rows = flat(idx[g].astype(jnp.float32)).astype(jnp.int32)
        idx_f[g] = rows
        idx_tx[g] = rows[early:]
    for g in range(2):
        live = slot_of < cnt[g : g + 1, :]
        wgt_f[g] = flat(jnp.where(live, wgt[g], 0.0))
        val_f[g] = flat(val[g])

    idx_copies = []
    for d, p in enumerate(peers):
        idx_copies.append(
            pltpu.make_async_remote_copy(
                idx_tx, idx_in.at[d], idx_s.at[d], idx_r.at[d], device_id={"mem": p}, device_id_type=MESH
            )
        )
        idx_copies[-1].start()
    start(moves[1:first])

    def gather(s, index):
        rows = s.shape[0]
        lane = lax.broadcasted_iota(jnp.int32, (rows, LANES), 1) // 16
        s = s.astype(jnp.float32)
        index = jnp.broadcast_to(index, (rows, LANES))
        picked = None
        for j in range(8):
            here = jnp.take_along_axis(s[:, j * LANES : (j + 1) * LANES], index, axis=1)
            picked = here if picked is None else jnp.where(lane == j, here, picked)
        return picked

    def lanes_of(unit):
        return pl.ds(pl.multiple_of(unit * LANES, LANES), LANES)

    def unit_cols(unit):
        return pl.ds(pl.multiple_of(unit * UNIT, LANES), UNIT)

    def take(x, index):
        return jnp.take_along_axis(x, jnp.broadcast_to(index, x.shape), axis=1)

    shape = (late * 8, LANES)
    lane = lax.broadcasted_iota(jnp.int32, shape, 1)
    block = lax.rem(lax.broadcasted_iota(jnp.int32, shape, 0), 8)
    lane_f = lane.astype(jnp.float32)
    upto = (
        lax.broadcasted_iota(jnp.int32, (LANES, LANES), 0)
        <= lax.broadcasted_iota(jnp.int32, (LANES, LANES), 1)
    ).astype(jnp.bfloat16)

    def spread(rows):
        return jnp.broadcast_to(rows[:, None, :], (late, 8, LANES)).reshape(shape)

    def own_slots(x):
        return jnp.sum(jnp.where(block == lane // 16, x, 0.0).reshape(late, 8, LANES), axis=1)

    def ranks(table):
        seen = jnp.zeros(shape, jnp.float32)
        for s in range(16):
            column = jnp.take_along_axis(table, block * 16 + s, axis=1)
            seen = jnp.where(column == lane_f, 1.0, seen)
        before = jnp.dot(seen.astype(jnp.bfloat16), upto, preferred_element_type=jnp.float32)
        spare = 16.0 - before[:, LANES - 1 :]
        other = lane_f + 1.0 - before
        ahead = before + jnp.minimum(other, spare)
        return (seen > 0.0) | (other <= spare), ahead, lane_f + 1.0 - ahead

    def search(rank, limit):
        at = jnp.zeros(shape, jnp.int32)
        for b in (64, 32, 16, 8, 4, 2, 1):
            here = jnp.take_along_axis(rank, at + (b - 1), axis=1)
            at = jnp.where(here <= limit, at + b, at)
        return at

    for g in range(2):
        table = spread(idx_tx[g].astype(jnp.float32))
        goes, ahead, behind = ranks(table)
        place = jnp.where(goes, (16 * block).astype(jnp.float32) + ahead - 1.0, LANES + behind - 1.0)
        back[g] = place.astype(jnp.int32)
        slots = own_slots(jnp.take_along_axis(ahead, table.astype(jnp.int32), axis=1))
        first_lane = (lax.broadcasted_iota(jnp.int32, (late, LANES), 1) // 16) * 16
        at_s[g] = slots.astype(jnp.int32) - 1 + first_lane

    for c in loads:
        c.wait()
    for c in idx_copies:
        c.wait()
    tail = lax.broadcasted_iota(jnp.int32, (mk, LANES), 1) >= 112

    def send_to(d, _):
        for g in range(2):
            table = spread(idx_in[nmem - 2 - d, g].astype(jnp.float32))
            _, ahead, behind = ranks(table)
            from_s[g] = own_slots(search(ahead, lax.rem(lane, 16).astype(jnp.float32)).astype(jnp.float32)).astype(jnp.int32)
            source = search(behind, lane_f)
            last = spread(source.astype(jnp.float32).reshape(late, 8, LANES)[:, 7, :])
            last = jnp.take_along_axis(last, jnp.clip(16 * block + lane - 112, 0, LANES - 1), axis=1)
            from_c[g] = jnp.where(lane < 112, source, last.astype(jnp.int32))

        def send_row(u, _):
            for g in range(2):
                x = stage[d, g, :, unit_cols(u)].astype(jnp.float32)
                tx[d, g, :, lanes_of(u)] = gather(x, from_s[g, pl.ds(u, 1), :]).astype(jnp.bfloat16)
                rest = []
                for t in range(7):
                    index = from_c[g, pl.ds(u * 8 + t, 1), :]
                    rest.append(
                        jnp.where(tail, take(x[:, 7 * LANES :], index), take(x[:, t * LANES : (t + 1) * LANES], index))
                    )
                where = pl.ds(pl.multiple_of(u * REST, LANES), REST)
                rest_tx[d, g, :, where] = jnp.concatenate(rest, axis=1).astype(jnp.bfloat16)
            return 0

        lax.fori_loop(0, late, send_row, 0)
        return 0

    lax.fori_loop(0, nmem - 1, send_to, 0)
    hx_copies = []
    for d, p in enumerate(peers):
        hx_copies.append(
            pltpu.make_async_remote_copy(
                tx.at[d], ahead_in.at[me], hx_s.at[d], hx_r.at[d], device_id={"mem": p}, device_id_type=MESH
            )
        )
    for c in own:
        c.wait()
    for g in range(2):

        def own_row(u, _):
            picked = gather(out[g][my_rows, unit_cols(early + u)], idx_f[g, pl.ds(early + u, 1), :])
            hx[me, g, :, lanes_of(u)] = picked.astype(jnp.bfloat16)
            return 0

        lax.fori_loop(0, late, own_row, 0)
    for c in hx_copies:
        c.start()
    start(moves[first:])

    def product(acc, x, value, weight):
        hmean = jnp.sum(x, axis=0, keepdims=True) / members
        rest = jnp.zeros((ROWS - members - 1, x.shape[1]), jnp.float32)
        aug = jnp.concatenate([x - hmean, value - hmean, rest], axis=0)
        return acc + lax.dot_general(
            aug * weight, aug, (((1,), (1,)), ((), ())), precision=HIGH,
            preferred_element_type=jnp.float32,
        )

    def early_sum(u, acc):
        for n, (at, _) in enumerate(early_moves):

            @pl.when(u == at)
            def _():
                for m in moves[n]:
                    m.wait_recv()

        x = [gather(out[g][:, unit_cols(u)], idx_f[g, pl.ds(u, 1), :]) for g in range(2)]
        value = [val_f[g, pl.ds(u, 1), :] for g in range(2)]
        weight = [wgt_f[g, pl.ds(u, 1), :] for g in range(2)]
        return product(acc, *(jnp.concatenate(t, axis=1) for t in (x, value, weight)))

    acc = lax.fori_loop(0, early - 1, early_sum, jnp.zeros((ROWS, ROWS), jnp.float32))
    for c in hx_copies:
        c.wait()

    def arrange(n, _):
        p = lax.rem(me + 1 + n // late, nmem)
        u = lax.rem(n, late)
        for g in range(2):
            x = ahead_in[p, g, :, lanes_of(u)].astype(jnp.float32)
            hx[p, g, :, lanes_of(u)] = take(x, at_s[g, pl.ds(u, 1), :]).astype(jnp.bfloat16)
        return 0

    lax.fori_loop(0, (nmem - 1) * late, arrange, 0)

    def late_sum(u, acc):
        x, value, weight = [], [], []
        for g in range(2):
            x.append(
                jnp.concatenate([hx[m, g, :, lanes_of(u)].astype(jnp.float32) for m in range(nmem)], axis=0)
            )
            value.append(val_f[g, pl.ds(early + u, 1), :])
            weight.append(wgt_f[g, pl.ds(early + u, 1), :])
        return product(acc, *(jnp.concatenate(t, axis=1) for t in (x, value, weight)))

    acc = lax.fori_loop(0, late, late_sum, acc)
    acc = early_sum(early - 1, acc)

    live = cnt[...].astype(jnp.float32)
    live = jnp.sum(jnp.sum(live, axis=1, keepdims=True), axis=0, keepdims=True)
    acc = pack(acc, live, members)

    def to_mate(n, src, dst):
        return pltpu.make_async_remote_copy(
            src, dst, pair_s.at[n], pair_r.at[n], device_id=mate, device_id_type=MESH
        )

    @pl.when(hub)
    def _():
        total = acc
        if paired:
            to_mate(0, res, got.at[0]).wait_recv()
            total = total + got[0]
        slot = 1
        for n, r in enumerate(rounds):
            cur[n] = total
            copies = []
            for p in r:
                copies.append(
                    pltpu.make_async_remote_copy(
                        cur.at[n], got.at[slot + len(copies)],
                        red_s.at[slot + len(copies)], red_r.at[slot + len(copies)],
                        device_id=partner(p), device_id_type=MESH,
                    )
                )
            for c in copies:
                c.start()
            for c in copies:
                c.wait()
            total = total + got[slot]
            if len(r) == 3:
                total = total + (got[slot + 1] + got[slot + 2])
            slot += len(r)
        res[...] = total
        if paired:
            to_mate(1, res, res).start()

    @pl.when(jnp.logical_not(hub))
    def _():
        cur[0] = acc
        pl.semaphore_wait(known, 1)
        send = to_mate(0, cur.at[0], got.at[0])
        send.start()
        send.wait_send()
        to_mate(1, res, res).wait_recv()

    weights = transform_of(res[...], members)
    tr[...] = weights
    left, coef = mixing(weights)
    lhs[...] = left
    count, width = tiles(early * UNIT)

    def mix_tile(i, _):
        where = pl.ds(pl.multiple_of(i * width, LANES), width)
        for g in range(2):
            out[g][:, where] = mix(lhs[...], coef, out[g][:, where])
        return 0

    lax.fori_loop(0, count, mix_tile, 0)
    low = lax.broadcasted_iota(jnp.int32, (mk, LANES), 1)

    def unpack(n, _):
        p = lax.rem(me + 1 + lax.rem(n, nmem - 1), nmem)
        u = n // (nmem - 1)
        for g in range(2):
            some = ahead_in[p, g, :, lanes_of(u)].astype(jnp.float32)
            rest = rest_in[p, g, :, pl.ds(pl.multiple_of(u * REST, LANES), REST)].astype(jnp.float32)
            rest = [rest[:, t * LANES : (t + 1) * LANES] for t in range(7)]
            last = None
            for t in range(7):
                here = jnp.take_along_axis(rest[t], 112 + lax.rem(low, 16), axis=1)
                last = here if last is None else jnp.where(low // 16 == t, here, last)
            blocks = []
            for t, other in enumerate(rest + [last]):
                index = jnp.broadcast_to(back[g, pl.ds(u * 8 + t, 1), :], (mk, LANES))
                inner = jnp.where(index < LANES, index, index - LANES)
                blocks.append(jnp.where(index < LANES, take(some, inner), take(other, inner)))
            rows = pl.ds(pl.multiple_of(p * mk, mk), mk)
            out[g][rows, unit_cols(early + u)] = jnp.concatenate(blocks, axis=1).astype(jnp.bfloat16)
        return 0

    for (at, size), ms in zip(late_moves, moves[len(early_moves) :]):
        for m in ms:
            m.wait_recv()
        begin = (at - early) * (nmem - 1)
        lax.fori_loop(begin, begin + size * (nmem - 1), unpack, 0)
    for ms in moves:
        for m in ms:
            m.wait_send()

    @pl.when(hub)
    def _():
        if paired:
            to_mate(1, res, res).wait_send()


def exchange(state_a, state_b, idx, val, wgt, cnt):
    nmem, ncol = lax.axis_size("mem"), lax.axis_size("col")
    mk, held = state_a.shape
    piece = held // nmem
    members = mk * nmem
    units, early_moves, late_moves = plan(piece)
    late = units - late_moves[0][0]
    rounds = sum_rounds(nmem, ncol)
    slots = 1 + sum(len(r) for r in rounds)
    moves = 2 * (nmem - 1) * len(early_moves + late_moves)
    used = members * members // LANES + 8
    dma = pltpu.SemaphoreType.DMA
    hbm = pl.BlockSpec(memory_space=pltpu.HBM)
    vmem = pl.BlockSpec(memory_space=pltpu.VMEM)
    return pl.pallas_call(
        functools.partial(exchange_kernel, nmem, ncol),
        out_shape=(
            pltpu.VMEM((members, piece), jnp.bfloat16),
            pltpu.VMEM((members, piece), jnp.bfloat16),
            pltpu.VMEM((members, members), jnp.float32),
        ),
        in_specs=[hbm] * 6,
        out_specs=(vmem, vmem, vmem),
        scratch_shapes=[
            *(pltpu.VMEM(x.shape, x.dtype) for x in (idx, val, wgt, cnt)),
            dma((4,)),
            pltpu.VMEM((nmem - 1, 2, mk, late * UNIT), jnp.bfloat16),
            pltpu.VMEM((2, units, LANES), jnp.int32),
            pltpu.VMEM((2, units, LANES), jnp.float32),
            pltpu.VMEM((2, units, LANES), jnp.float32),
            pltpu.VMEM((2, late, LANES), jnp.int32),
            pltpu.VMEM((nmem - 1, 2, late, LANES), jnp.int32),
            pltpu.VMEM((2, late, LANES), jnp.int32),
            pltpu.VMEM((2, late * 8, LANES), jnp.int32),
            pltpu.VMEM((2, late, LANES), jnp.int32),
            pltpu.VMEM((2, late * 8, LANES), jnp.int32),
            pltpu.VMEM((nmem - 1, 2, mk, late * LANES), jnp.bfloat16),
            pltpu.VMEM((nmem - 1, 2, mk, late * REST), jnp.bfloat16),
            pltpu.VMEM((nmem, 2, mk, late * LANES), jnp.bfloat16),
            pltpu.VMEM((nmem, 2, mk, late * REST), jnp.bfloat16),
            pltpu.VMEM((nmem, 2, mk, late * LANES), jnp.bfloat16),
            pltpu.VMEM((max(1, len(rounds)), used, LANES), jnp.float32),
            pltpu.VMEM((slots, used, LANES), jnp.float32),
            pltpu.VMEM((used, LANES), jnp.float32),
            pltpu.VMEM((members + 16, members), jnp.bfloat16),
            dma((2,)),
            dma((nmem - 1, 2)),
            dma((nmem - 1,)),
            dma((nmem - 1,)),
            dma((nmem - 1,)),
            dma((nmem - 1,)),
            dma((moves,)),
            dma((moves,)),
            dma((slots,)),
            dma((slots,)),
            dma((2,)),
            dma((2,)),
            pltpu.SemaphoreType.REGULAR,
        ],
        compiler_params=pltpu.CompilerParams(
            collective_id=0, has_side_effects=True, vmem_limit_bytes=40 * 2**20
        ),
        name="exchange",
    )(*(pltpu.with_memory_space_constraint(x, pltpu.HBM) for x in (state_a, state_b, idx, val, wgt, cnt)))


def write_kernel(early, xa, xb, tr, oa, ob, ot, mixed, early_sem, late_sem, tr_sem):
    copies = [pltpu.make_async_copy(tr, ot, tr_sem)]
    count = early_sem.shape[1]
    for i in range(count):
        for g, (x, o) in enumerate(((xa, oa), (xb, ob))):
            where = pl.ds(i * (early // count), early // count)
            copies.append(pltpu.make_async_copy(x.at[:, where], o.at[:, where], early_sem.at[g, i]))
    for c in copies:
        c.start()
    lhs, coef = mixing(tr[...])
    width = mixed.shape[3]
    for i in range(mixed.shape[0]):
        for g, (x, o) in enumerate(((xa, oa), (xb, ob))):
            where = pl.ds(early + i * width, width)
            mixed[i, g] = mix(lhs, coef, x[:, where])
            copies.append(pltpu.make_async_copy(mixed.at[i, g], o.at[:, where], late_sem.at[g, i]))
            copies[-1].start()
    for c in copies:
        c.wait()


def write(xa, xb, tr):
    members, piece = xa.shape
    early = plan(piece)[2][0][0] * UNIT
    count, width = tiles(piece - early)
    parts = 2
    vmem = pl.BlockSpec(memory_space=pltpu.VMEM)
    hbm = pl.BlockSpec(memory_space=pltpu.HBM)
    dma = pltpu.SemaphoreType.DMA
    return pl.pallas_call(
        functools.partial(write_kernel, early),
        out_shape=tuple(jax.ShapeDtypeStruct(x.shape, x.dtype) for x in (xa, xb, tr)),
        in_specs=[vmem, vmem, vmem],
        out_specs=(hbm, hbm, hbm),
        scratch_shapes=[
            pltpu.VMEM((count, 2, members, width), xa.dtype),
            dma((2, parts)),
            dma((2, count)),
            dma,
        ],
        compiler_params=pltpu.CompilerParams(vmem_limit_bytes=40 * 2**20),
        name="write",
    )(xa, xb, tr)


def shards(state_a, state_b, obs_index, observation_count, obs_value, obs_weight):
    tables = [jnp.transpose(x, (0, 2, 1)) for x in (obs_index, obs_value, obs_weight)]
    return write(*exchange(state_a, state_b, *tables, observation_count))


def solution(mesh):
    return jax.shard_map(
        shards,
        mesh=mesh,
        in_specs=(
            P("mem", "col"),
            P("mem", "col"),
            P(None, ("col", "mem"), None),
            P(None, ("col", "mem")),
            P(None, ("col", "mem"), None),
            P(None, ("col", "mem"), None),
        ),
        out_specs=(P(None, ("col", "mem")), P(None, ("col", "mem")), P()),
        check_vma=False,
    )
```

```python
import functools

import jax
import jax.numpy as jnp
from jax import lax
from jax.experimental import pallas as pl
from jax.experimental.pallas import tpu as pltpu
from jax.sharding import PartitionSpec as P

ITERS = 24
LANES = 128
HIGH = lax.Precision.HIGHEST
MESH = pl.DeviceIdType.MESH
ROWS = 128
UNIT = 1024
LATE = 0.5
FIRST = 16
EARLY_SIZES = (1, 2, 4)
LATE_SIZES = (1, 2, 4)
REST = UNIT - LANES
WIDE = 6144


def bits(n):
    return [1 << i for i in range(n.bit_length() - 1)]


def pack(sums, live, members):
    height = members * members // LANES
    rows = [sums[i : i + height, :members] for i in range(0, members, height)]
    lane = lax.broadcasted_iota(jnp.int32, (1, LANES), 1)
    last = jnp.where(lane == members + 1, live, sums[members : members + 1])
    return jnp.concatenate([jnp.concatenate(rows, axis=1), last, jnp.zeros((7, LANES), jnp.float32)], axis=0)


def transform_of(packed, members):
    height = members * members // LANES
    g = jnp.concatenate([packed[:height, i : i + members] for i in range(0, LANES, members)], axis=0)
    last = packed[height : height + 1]
    cross, misfit, total = last[:, :members], last[:, members : members + 1], last[:, members + 1 : members + 2]
    rows = lax.broadcasted_iota(jnp.int32, (members, members), 0)
    cols = lax.broadcasted_iota(jnp.int32, (members, members), 1)
    eye = (rows == cols).astype(jnp.float32)

    def whole(x):
        return jnp.sum(jnp.sum(x, axis=1, keepdims=True), axis=0, keepdims=True)

    def parts(x):
        hi = x.astype(jnp.bfloat16)
        rest = x - hi.astype(jnp.float32)
        mid = rest.astype(jnp.bfloat16)
        low = (rest - mid.astype(jnp.float32)).astype(jnp.bfloat16)
        return hi, mid, low

    def dot(a, b):
        total = None
        for i in range(3):
            left = jnp.concatenate(a[: 3 - i], axis=0) if i < 2 else a[0]
            out = jnp.dot(left, b[i], preferred_element_type=jnp.float32)
            for j in reversed(range(3 - i)):
                block = out[j * members : (j + 1) * members]
                total = block if total is None else total + block
        return total

    dof = members - 1.0
    scl = dof / total
    gs = scl * g
    bs = scl * cross
    rho = (1.0 + scl * misfit / dof) / (1.0 + whole(gs * eye) / dof)
    amat = dof / rho * eye + gs
    scale = jnp.sqrt(whole(amat * amat))

    def step(_, carry):
        yn, zn = carry
        yp, zp = parts(yn), parts(zn)
        tp = parts(1.5 * eye - 0.5 * dot(zp, yp))
        return dot(yp, tp), dot(tp, zp)

    _, zn = lax.fori_loop(0, ITERS, step, (amat / scale, eye))
    zp = parts(zn)
    wbar = jnp.sum(dot(zp, zp) / scale * bs, axis=1, keepdims=True)
    return jnp.sqrt(dof) * zn / jnp.sqrt(scale) + wbar


def cut(units, sizes):
    out = []
    while units:
        out.insert(0, min(units, sizes[min(len(out), len(sizes) - 1)]))
        units -= out[0]
    return out


def plan(piece):
    units = piece // UNIT
    late = max(1, round(units * LATE))
    at, moves = 0, []
    for part in cut(units - late, EARLY_SIZES), cut(late, LATE_SIZES):
        moves.append([])
        for n in part:
            moves[-1].append((at, n))
            at += n
    return units, *moves


def mixed_units(late_moves):
    return late_moves[-2:][0][0]


def tiles(columns):
    n = 1
    while columns % (n * LANES) or columns // n > WIDE:
        n += 1
    return n, columns // n


def mixing(tr):
    members = tr.shape[0]
    wt = tr.T.astype(jnp.bfloat16)
    mean = jnp.full((16, members), 1.0 / members, jnp.bfloat16)
    return jnp.concatenate([wt, mean], axis=0), 1.0 - jnp.sum(wt.astype(jnp.float32), axis=1, keepdims=True)


def mix(lhs, coef, x):
    members = x.shape[0]
    mixed = jnp.dot(lhs, x, preferred_element_type=jnp.float32)
    return (mixed[:members] + coef * mixed[members : members + 1]).astype(x.dtype)


def sum_rounds(nmem, ncol):
    aside = 4 if ncol > 4 else 0
    rounds = [[(b, aside)] for b in bits(nmem)]
    gens = [(0, b) for b in bits(ncol) if b > 1]
    for i in range(0, len(gens), 2):
        pair = gens[i : i + 2]
        if len(pair) == 2:
            pair.append((0, pair[0][1] ^ pair[1][1]))
        rounds.append(pair)
    return rounds


def take(x, index):
    return jnp.take_along_axis(x, jnp.broadcast_to(index, x.shape), axis=1)


def unpack(some, rest, back):
    some, rest = some.astype(jnp.float32), rest.astype(jnp.float32)
    rest = [rest[:, t * LANES : (t + 1) * LANES] for t in range(7)]
    lane = lax.broadcasted_iota(jnp.int32, some.shape, 1)
    last = None
    for t in range(7):
        here = jnp.take_along_axis(rest[t], 112 + lax.rem(lane, 16), axis=1)
        last = here if last is None else jnp.where(lane // 16 == t, here, last)
    blocks = []
    for t, other in enumerate(rest + [last]):
        index = jnp.broadcast_to(back[t : t + 1], some.shape)
        inner = jnp.where(index < LANES, index, index - LANES)
        blocks.append(jnp.where(index < LANES, take(some, inner), take(other, inner)))
    return jnp.concatenate(blocks, axis=1).astype(jnp.bfloat16)


def exchange_kernel(
    nmem, ncol, sa, sb, idx_hbm, val_hbm, wgt_hbm, cnt_hbm, oa, ob, tr, some_out, rest_out, back_out,
    idx, val, wgt, cnt, table_sem, stage, idx_f, val_f, wgt_f, idx_tx, idx_in,
    from_s, from_c, at_s, back, tx, rest_tx, ahead_in, rest_in, hx, cur, got, res, lhs,
    own_sem, stage_sem, idx_s, idx_r, hx_s, hx_r, st_s, st_r, red_s, red_r, pair_s, pair_r, known,
):
    me = lax.axis_index("mem")
    col = lax.axis_index("col")
    mk = sa.shape[0]
    members = mk * nmem
    piece = sa.shape[1] // nmem
    nblk = idx.shape[2]
    units, early_moves, late_moves = plan(piece)
    early = late_moves[0][0]
    late = units - early
    state, out = (sa, sb), (oa, ob)
    peers = [lax.rem(me + d, nmem) for d in range(1, nmem)]
    rounds = sum_rounds(nmem, ncol)
    greeted = sorted({p for r in rounds for p in r if p[1]})
    paired = ncol > 1
    mate = {"col": col ^ 1}
    hub = lax.rem(col, 2) == 0

    def partner(p):
        return {"mem": me ^ p[0], "col": col ^ p[1]}

    def cols_of(owner, unit, size):
        return pl.ds(pl.multiple_of(owner * piece + unit * UNIT, LANES), size * UNIT)

    my_rows = pl.ds(pl.multiple_of(me * mk, mk), mk)

    loads = []
    for d, p in enumerate(peers):
        for g in range(2):
            loads.append(
                pltpu.make_async_copy(
                    state[g].at[:, cols_of(p, early, late)], stage.at[d, g], stage_sem.at[d, g]
                )
            )
    own = []
    for g in range(2):
        own.append(
            pltpu.make_async_copy(
                state[g].at[:, cols_of(me, 0, units)], out[g].at[my_rows, :], own_sem.at[g]
            )
        )
    tables = []
    for n, (a, b) in enumerate(((idx_hbm, idx), (val_hbm, val), (wgt_hbm, wgt), (cnt_hbm, cnt))):
        tables.append(pltpu.make_async_copy(a, b, table_sem.at[n]))
    for c in tables:
        c.start()

    barrier = pltpu.get_barrier_semaphore()
    for p in peers:
        pl.semaphore_signal(barrier, inc=1, device_id={"mem": p}, device_id_type=MESH)
    @pl.when(hub)
    def _():
        for p in greeted:
            pl.semaphore_signal(barrier, inc=1, device_id=partner(p), device_id_type=MESH)
        pl.semaphore_wait(barrier, len(peers) + len(greeted) + paired)
        if paired:
            pl.semaphore_signal(known, inc=1, device_id=mate, device_id_type=MESH)

    @pl.when(jnp.logical_not(hub))
    def _():
        pl.semaphore_signal(barrier, inc=1, device_id=mate, device_id_type=MESH)
        pl.semaphore_wait(barrier, len(peers))

    each = [(g, d) for g in range(2) for d in range(nmem - 1)]
    moves = []
    for at, size in early_moves + late_moves:
        moves.append([])
        for g, d in each:
            slot = (len(moves) - 1) * len(each) + len(moves[-1])
            if at < early:
                source = state[g].at[:, cols_of(peers[d], at, size)]
                target = out[g].at[my_rows, pl.ds(at * UNIT, size * UNIT)]
            else:
                where = pl.ds((at - early) * REST, size * REST)
                source, target = rest_tx.at[d, g, :, where], rest_in.at[me, g, :, where]
                if (at, size) == late_moves[-1]:
                    target = rest_out.at[me, g]
            moves[-1].append(
                pltpu.make_async_remote_copy(
                    source, target, st_s.at[slot], st_r.at[slot],
                    device_id={"mem": peers[d]}, device_id_type=MESH,
                )
            )
    first = len([at for at, _ in early_moves if 0 < at < FIRST]) + 1

    def start(some):
        for ms in some:
            for m in ms:
                m.start()

    start(moves[:1])
    for c in loads + own:
        c.start()

    for c in tables:
        c.wait()
    slot_of = lax.broadcasted_iota(jnp.int32, (16, nblk), 0)
    diag = (
        lax.broadcasted_iota(jnp.int32, (8, LANES), 0)
        == lax.broadcasted_iota(jnp.int32, (8, LANES), 1) // 16
    )

    def flat(x):
        x = jnp.concatenate([x] * 8, axis=0).T.reshape(units, 8, LANES)
        return jnp.sum(jnp.where(diag[None], x, 0.0), axis=1)

    for g in range(2):
        rows = flat(idx[g].astype(jnp.float32))
        idx_f[g] = rows.astype(jnp.int32)
        idx_tx[g] = rows[early:].astype(jnp.bfloat16)
    for g in range(2):
        live = slot_of < cnt[g : g + 1, :]
        wgt_f[g] = flat(jnp.where(live, wgt[g], 0.0))
        val_f[g] = flat(val[g])

    idx_copies = []
    for d, p in enumerate(peers):
        idx_copies.append(
            pltpu.make_async_remote_copy(
                idx_tx, idx_in.at[d], idx_s.at[d], idx_r.at[d], device_id={"mem": p}, device_id_type=MESH
            )
        )
        idx_copies[-1].start()
    start(moves[1:first])

    def gather(s, index):
        rows = s.shape[0]
        lane = lax.broadcasted_iota(jnp.int32, (rows, LANES), 1) // 16
        s = s.astype(jnp.float32)
        index = jnp.broadcast_to(index, (rows, LANES))
        picked = None
        for j in range(8):
            here = jnp.take_along_axis(s[:, j * LANES : (j + 1) * LANES], index, axis=1)
            picked = here if picked is None else jnp.where(lane == j, here, picked)
        return picked

    def lanes_of(unit):
        return pl.ds(pl.multiple_of(unit * LANES, LANES), LANES)

    def unit_cols(unit):
        return pl.ds(pl.multiple_of(unit * UNIT, LANES), UNIT)

    shape = (late * 8, LANES)
    lane = lax.broadcasted_iota(jnp.int32, shape, 1)
    block = lax.rem(lax.broadcasted_iota(jnp.int32, shape, 0), 8)
    lane_f = lane.astype(jnp.float32)
    upto = (
        lax.broadcasted_iota(jnp.int32, (LANES, LANES), 0)
        <= lax.broadcasted_iota(jnp.int32, (LANES, LANES), 1)
    ).astype(jnp.bfloat16)

    def spread(rows):
        return jnp.broadcast_to(rows[:, None, :], (late, 8, LANES)).reshape(shape)

    def own_slots(x):
        return jnp.sum(jnp.where(block == lane // 16, x, 0.0).reshape(late, 8, LANES), axis=1)

    def ranks(table):
        seen = jnp.zeros(shape, jnp.float32)
        for s in range(16):
            column = jnp.take_along_axis(table, block * 16 + s, axis=1)
            seen = jnp.where(column == lane_f, 1.0, seen)
        before = jnp.dot(seen.astype(jnp.bfloat16), upto, preferred_element_type=jnp.float32)
        spare = 16.0 - before[:, LANES - 1 :]
        other = lane_f + 1.0 - before
        ahead = before + jnp.minimum(other, spare)
        return (seen > 0.0) | (other <= spare), ahead, lane_f + 1.0 - ahead

    def search(rank, limit):
        at = jnp.zeros(shape, jnp.int32)
        for b in (64, 32, 16, 8, 4, 2, 1):
            here = jnp.take_along_axis(rank, at + (b - 1), axis=1)
            at = jnp.where(here <= limit, at + b, at)
        return at

    for g in range(2):
        table = spread(idx_tx[g].astype(jnp.float32))
        goes, ahead, behind = ranks(table)
        place = jnp.where(goes, (16 * block).astype(jnp.float32) + ahead - 1.0, LANES + behind - 1.0)
        back[g] = place.astype(jnp.int32)
        back_out[g] = place[(late_moves[-1][0] - early) * 8 :].astype(jnp.int32)
        slots = own_slots(jnp.take_along_axis(ahead, table.astype(jnp.int32), axis=1))
        first_lane = (lax.broadcasted_iota(jnp.int32, (late, LANES), 1) // 16) * 16
        at_s[g] = slots.astype(jnp.int32) - 1 + first_lane

    for c in loads:
        c.wait()
    for c in idx_copies:
        c.wait()
    tail = lax.broadcasted_iota(jnp.int32, (mk, LANES), 1) >= 112

    def send_to(d, _):
        for g in range(2):
            table = spread(idx_in[nmem - 2 - d, g].astype(jnp.float32))
            _, ahead, behind = ranks(table)
            from_s[g] = own_slots(search(ahead, lax.rem(lane, 16).astype(jnp.float32)).astype(jnp.float32)).astype(jnp.int32)
            source = search(behind, lane_f)
            last = spread(source.astype(jnp.float32).reshape(late, 8, LANES)[:, 7, :])
            last = jnp.take_along_axis(last, jnp.clip(16 * block + lane - 112, 0, LANES - 1), axis=1)
            from_c[g] = jnp.where(lane < 112, source, last.astype(jnp.int32))

        def send_row(u, _):
            for g in range(2):
                x = stage[d, g, :, unit_cols(u)].astype(jnp.float32)
                tx[d, g, :, lanes_of(u)] = gather(x, from_s[g, pl.ds(u, 1), :]).astype(jnp.bfloat16)
                rest = []
                for t in range(7):
                    index = from_c[g, pl.ds(u * 8 + t, 1), :]
                    rest.append(
                        jnp.where(tail, take(x[:, 7 * LANES :], index), take(x[:, t * LANES : (t + 1) * LANES], index))
                    )
                where = pl.ds(pl.multiple_of(u * REST, LANES), REST)
                rest_tx[d, g, :, where] = jnp.concatenate(rest, axis=1).astype(jnp.bfloat16)
            return 0

        lax.fori_loop(0, late, send_row, 0)
        return 0

    lax.fori_loop(0, nmem - 1, send_to, 0)
    hx_copies = []
    for d, p in enumerate(peers):
        hx_copies.append(
            pltpu.make_async_remote_copy(
                tx.at[d], ahead_in.at[me], hx_s.at[d], hx_r.at[d], device_id={"mem": p}, device_id_type=MESH
            )
        )
    for c in own:
        c.wait()
    for g in range(2):

        def own_row(u, _):
            picked = gather(out[g][my_rows, unit_cols(early + u)], idx_f[g, pl.ds(early + u, 1), :])
            hx[me, g, :, lanes_of(u)] = picked.astype(jnp.bfloat16)
            return 0

        lax.fori_loop(0, late, own_row, 0)
    for c in hx_copies:
        c.start()
    start(moves[first:])

    def product(acc, x, value, weight):
        hmean = jnp.sum(x, axis=0, keepdims=True) / members
        rest = jnp.zeros((ROWS - members - 1, x.shape[1]), jnp.float32)
        aug = jnp.concatenate([x - hmean, value - hmean, rest], axis=0)
        return acc + lax.dot_general(
            aug * weight, aug, (((1,), (1,)), ((), ())), precision=HIGH,
            preferred_element_type=jnp.float32,
        )

    def early_sum(u, acc):
        for n, (at, _) in enumerate(early_moves):

            @pl.when(u == at)
            def _():
                for m in moves[n]:
                    m.wait_recv()

        x = [gather(out[g][:, unit_cols(u)], idx_f[g, pl.ds(u, 1), :]) for g in range(2)]
        value = [val_f[g, pl.ds(u, 1), :] for g in range(2)]
        weight = [wgt_f[g, pl.ds(u, 1), :] for g in range(2)]
        return product(acc, *(jnp.concatenate(t, axis=1) for t in (x, value, weight)))

    acc = lax.fori_loop(0, early - 1, early_sum, jnp.zeros((ROWS, ROWS), jnp.float32))
    for c in hx_copies:
        c.wait()

    def arrange(n, _):
        p = lax.rem(me + 1 + n // late, nmem)
        u = lax.rem(n, late)
        for g in range(2):
            x = ahead_in[p, g, :, lanes_of(u)].astype(jnp.float32)
            hx[p, g, :, lanes_of(u)] = take(x, at_s[g, pl.ds(u, 1), :]).astype(jnp.bfloat16)
        return 0

    lax.fori_loop(0, (nmem - 1) * late, arrange, 0)
    some_out[...] = ahead_in[:, :, :, (late_moves[-1][0] - early) * LANES :]

    def late_sum(u, acc):
        x, value, weight = [], [], []
        for g in range(2):
            x.append(
                jnp.concatenate([hx[m, g, :, lanes_of(u)].astype(jnp.float32) for m in range(nmem)], axis=0)
            )
            value.append(val_f[g, pl.ds(early + u, 1), :])
            weight.append(wgt_f[g, pl.ds(early + u, 1), :])
        return product(acc, *(jnp.concatenate(t, axis=1) for t in (x, value, weight)))

    acc = lax.fori_loop(0, late, late_sum, acc)
    acc = early_sum(early - 1, acc)

    live = cnt[...].astype(jnp.float32)
    live = jnp.sum(jnp.sum(live, axis=1, keepdims=True), axis=0, keepdims=True)
    acc = pack(acc, live, members)

    def to_mate(n, src, dst):
        return pltpu.make_async_remote_copy(
            src, dst, pair_s.at[n], pair_r.at[n], device_id=mate, device_id_type=MESH
        )

    @pl.when(hub)
    def _():
        total = acc
        if paired:
            to_mate(0, res, got.at[0]).wait_recv()
            total = total + got[0]
        slot = 1
        for n, r in enumerate(rounds):
            cur[n] = total
            copies = []
            for p in r:
                copies.append(
                    pltpu.make_async_remote_copy(
                        cur.at[n], got.at[slot + len(copies)],
                        red_s.at[slot + len(copies)], red_r.at[slot + len(copies)],
                        device_id=partner(p), device_id_type=MESH,
                    )
                )
            for c in copies:
                c.start()
            for c in copies:
                c.wait()
            total = total + got[slot]
            if len(r) == 3:
                total = total + (got[slot + 1] + got[slot + 2])
            slot += len(r)
        res[...] = total
        if paired:
            to_mate(1, res, res).start()

    @pl.when(jnp.logical_not(hub))
    def _():
        cur[0] = acc
        pl.semaphore_wait(known, 1)
        send = to_mate(0, cur.at[0], got.at[0])
        send.start()
        send.wait_send()
        to_mate(1, res, res).wait_recv()

    weights = transform_of(res[...], members)
    tr[...] = weights
    left, coef = mixing(weights)
    lhs[...] = left
    count, width = tiles(early * UNIT)

    def mix_tile(i, _):
        where = pl.ds(pl.multiple_of(i * width, LANES), width)
        for g in range(2):
            out[g][:, where] = mix(lhs[...], coef, out[g][:, where])
        return 0

    lax.fori_loop(0, count, mix_tile, 0)

    def put_back(n, _):
        p = lax.rem(me + 1 + lax.rem(n, nmem - 1), nmem)
        u = n // (nmem - 1)
        rows = pl.ds(pl.multiple_of(p * mk, mk), mk)
        for g in range(2):
            out[g][rows, unit_cols(early + u)] = unpack(
                ahead_in[p, g, :, lanes_of(u)],
                rest_in[p, g, :, pl.ds(pl.multiple_of(u * REST, LANES), REST)],
                back[g, pl.ds(pl.multiple_of(u * 8, 8), 8), :],
            )
        return 0

    for (at, size), ms in zip(late_moves, moves[len(early_moves) :]):
        for m in ms:
            m.wait_recv()
        if (at, size) != late_moves[-1]:
            begin = (at - early) * (nmem - 1)
            lax.fori_loop(begin, begin + size * (nmem - 1), put_back, 0)
        if at < mixed_units(late_moves):
            where = pl.ds(at * UNIT, size * UNIT)
            for g in range(2):
                out[g][:, where] = mix(lhs[...], coef, out[g][:, where])
    for ms in moves:
        for m in ms:
            m.wait_send()

    @pl.when(hub)
    def _():
        if paired:
            to_mate(1, res, res).wait_send()


def exchange(state_a, state_b, idx, val, wgt, cnt):
    nmem, ncol = lax.axis_size("mem"), lax.axis_size("col")
    mk, held = state_a.shape
    piece = held // nmem
    members = mk * nmem
    units, early_moves, late_moves = plan(piece)
    late = units - late_moves[0][0]
    rounds = sum_rounds(nmem, ncol)
    slots = 1 + sum(len(r) for r in rounds)
    moves = 2 * (nmem - 1) * len(early_moves + late_moves)
    used = members * members // LANES + 8
    dma = pltpu.SemaphoreType.DMA
    hbm = pl.BlockSpec(memory_space=pltpu.HBM)
    vmem = pl.BlockSpec(memory_space=pltpu.VMEM)
    return pl.pallas_call(
        functools.partial(exchange_kernel, nmem, ncol),
        out_shape=(
            pltpu.VMEM((members, piece), jnp.bfloat16),
            pltpu.VMEM((members, piece), jnp.bfloat16),
            pltpu.VMEM((members, members), jnp.float32),
            pltpu.VMEM((nmem, 2, mk, late_moves[-1][1] * LANES), jnp.bfloat16),
            pltpu.VMEM((nmem, 2, mk, late_moves[-1][1] * REST), jnp.bfloat16),
            pltpu.VMEM((2, late_moves[-1][1] * 8, LANES), jnp.int32),
        ),
        in_specs=[hbm] * 6,
        out_specs=(vmem,) * 6,
        scratch_shapes=[
            *(pltpu.VMEM(x.shape, x.dtype) for x in (idx, val, wgt, cnt)),
            dma((4,)),
            pltpu.VMEM((nmem - 1, 2, mk, late * UNIT), jnp.bfloat16),
            pltpu.VMEM((2, units, LANES), jnp.int32),
            pltpu.VMEM((2, units, LANES), jnp.float32),
            pltpu.VMEM((2, units, LANES), jnp.float32),
            pltpu.VMEM((2, late, LANES), jnp.bfloat16),
            pltpu.VMEM((nmem - 1, 2, late, LANES), jnp.bfloat16),
            pltpu.VMEM((2, late, LANES), jnp.int32),
            pltpu.VMEM((2, late * 8, LANES), jnp.int32),
            pltpu.VMEM((2, late, LANES), jnp.int32),
            pltpu.VMEM((2, late * 8, LANES), jnp.int32),
            pltpu.VMEM((nmem - 1, 2, mk, late * LANES), jnp.bfloat16),
            pltpu.VMEM((nmem - 1, 2, mk, late * REST), jnp.bfloat16),
            pltpu.VMEM((nmem, 2, mk, late * LANES), jnp.bfloat16),
            pltpu.VMEM((nmem, 2, mk, late * REST), jnp.bfloat16),
            pltpu.VMEM((nmem, 2, mk, late * LANES), jnp.bfloat16),
            pltpu.VMEM((max(1, len(rounds)), used, LANES), jnp.float32),
            pltpu.VMEM((slots, used, LANES), jnp.float32),
            pltpu.VMEM((used, LANES), jnp.float32),
            pltpu.VMEM((members + 16, members), jnp.bfloat16),
            dma((2,)),
            dma((nmem - 1, 2)),
            dma((nmem - 1,)),
            dma((nmem - 1,)),
            dma((nmem - 1,)),
            dma((nmem - 1,)),
            dma((moves,)),
            dma((moves,)),
            dma((slots,)),
            dma((slots,)),
            dma((2,)),
            dma((2,)),
            pltpu.SemaphoreType.REGULAR,
        ],
        compiler_params=pltpu.CompilerParams(
            collective_id=0, has_side_effects=True, vmem_limit_bytes=40 * 2**20
        ),
        name="exchange",
    )(*(pltpu.with_memory_space_constraint(x, pltpu.HBM) for x in (state_a, state_b, idx, val, wgt, cnt)))


def write_kernel(nmem, ready, xa, xb, tr, some, rest, back, oa, ob, ot, mid, end, sems, tr_sem):
    me = lax.axis_index("mem")
    mk = xa.shape[0] // nmem
    piece = xa.shape[1]
    last = end.shape[2]
    pairs = list(enumerate(((xa, oa), (xb, ob))))
    copies = [pltpu.make_async_copy(tr, ot, tr_sem)]
    half = ready // 2
    for i in range(2):
        for g, (x, o) in pairs:
            where = pl.ds(i * half, half)
            copies.append(pltpu.make_async_copy(x.at[:, where], o.at[:, where], sems.at[g, i]))
    for c in copies:
        c.start()

    def send(g, n, source, target):
        copies.append(pltpu.make_async_copy(source, target, sems.at[g, n]))
        copies[-1].start()

    lhs, coef = mixing(tr[...])
    if ready < piece - last:
        for g, (x, o) in pairs:
            where = pl.ds(ready, piece - last - ready)
            mid[g] = mix(lhs, coef, x[:, where])
            send(g, 2, mid.at[g], o.at[:, where])
    for g, (x, o) in pairs:
        where = pl.ds(piece - last, last)
        end[g] = x[:, where]
        for d in range(1, nmem):
            p = lax.rem(me + d, nmem)
            for u in range(last // UNIT):
                end[g, pl.ds(pl.multiple_of(p * mk, mk), mk), u * UNIT : (u + 1) * UNIT] = unpack(
                    some[p, g, :, u * LANES : (u + 1) * LANES],
                    rest[p, g, :, u * REST : (u + 1) * REST],
                    back[g, u * 8 : (u + 1) * 8, :],
                )
        end[g] = mix(lhs, coef, end[g])
        send(g, 3, end.at[g], o.at[:, where])
    for c in copies:
        c.wait()


def write(xa, xb, tr, some, rest, back):
    members, piece = xa.shape
    _, _, late_moves = plan(piece)
    ready, last = mixed_units(late_moves) * UNIT, late_moves[-1][1] * UNIT
    vmem = pl.BlockSpec(memory_space=pltpu.VMEM)
    hbm = pl.BlockSpec(memory_space=pltpu.HBM)
    return pl.pallas_call(
        functools.partial(write_kernel, some.shape[0], ready),
        out_shape=tuple(jax.ShapeDtypeStruct(x.shape, x.dtype) for x in (xa, xb, tr)),
        in_specs=[vmem] * 6,
        out_specs=(hbm, hbm, hbm),
        scratch_shapes=[
            pltpu.VMEM((2, members, max(LANES, piece - last - ready)), xa.dtype),
            pltpu.VMEM((2, members, last), xa.dtype),
            pltpu.SemaphoreType.DMA((2, 4)),
            pltpu.SemaphoreType.DMA,
        ],
        compiler_params=pltpu.CompilerParams(vmem_limit_bytes=40 * 2**20),
        name="write",
    )(xa, xb, tr, some, rest, back)


def shards(state_a, state_b, obs_index, observation_count, obs_value, obs_weight):
    tables = [jnp.transpose(x, (0, 2, 1)) for x in (obs_index, obs_value, obs_weight)]
    return write(*exchange(state_a, state_b, *tables, observation_count))


def solution(mesh):
    return jax.shard_map(
        shards,
        mesh=mesh,
        in_specs=(
            P("mem", "col"),
            P("mem", "col"),
            P(None, ("col", "mem"), None),
            P(None, ("col", "mem")),
            P(None, ("col", "mem"), None),
            P(None, ("col", "mem"), None),
        ),
        out_specs=(P(None, ("col", "mem")), P(None, ("col", "mem")), P()),
        check_vma=False,
    )
```

```python
import functools

import jax
import jax.numpy as jnp
from jax import lax
from jax.experimental import pallas as pl
from jax.experimental.pallas import tpu as pltpu
from jax.sharding import PartitionSpec as P

ITERS = 24
LANES = 128
HIGH = lax.Precision.HIGHEST
MESH = pl.DeviceIdType.MESH
ROWS = 128
UNIT = 1024
LATE = 0.5
FIRST = 16
EARLY_SIZES = (1, 3, 6)
LATE_SIZES = (2, 4, 6)
REST = UNIT - LANES
PARTS = 4
WIDE = 6144


def bits(n):
    return [1 << i for i in range(n.bit_length() - 1)]


def pack(sums, live, members):
    height = members * members // LANES
    rows = [sums[i : i + height, :members] for i in range(0, members, height)]
    lane = lax.broadcasted_iota(jnp.int32, (1, LANES), 1)
    last = jnp.where(lane == members + 1, live, sums[members : members + 1])
    return jnp.concatenate([jnp.concatenate(rows, axis=1), last, jnp.zeros((7, LANES), jnp.float32)], axis=0)


def transform_of(packed, members):
    height = members * members // LANES
    g = jnp.concatenate([packed[:height, i : i + members] for i in range(0, LANES, members)], axis=0)
    last = packed[height : height + 1]
    cross, misfit, total = last[:, :members], last[:, members : members + 1], last[:, members + 1 : members + 2]
    rows = lax.broadcasted_iota(jnp.int32, (members, members), 0)
    cols = lax.broadcasted_iota(jnp.int32, (members, members), 1)
    eye = (rows == cols).astype(jnp.float32)

    def whole(x):
        return jnp.sum(jnp.sum(x, axis=1, keepdims=True), axis=0, keepdims=True)

    def parts(x):
        hi = x.astype(jnp.bfloat16)
        rest = x - hi.astype(jnp.float32)
        mid = rest.astype(jnp.bfloat16)
        low = (rest - mid.astype(jnp.float32)).astype(jnp.bfloat16)
        return hi, mid, low

    def dot(a, b):
        total = None
        for i in range(3):
            left = jnp.concatenate(a[: 3 - i], axis=0) if i < 2 else a[0]
            out = jnp.dot(left, b[i], preferred_element_type=jnp.float32)
            for j in reversed(range(3 - i)):
                block = out[j * members : (j + 1) * members]
                total = block if total is None else total + block
        return total

    dof = members - 1.0
    scl = dof / total
    gs = scl * g
    bs = scl * cross
    rho = (1.0 + scl * misfit / dof) / (1.0 + whole(gs * eye) / dof)
    amat = dof / rho * eye + gs
    scale = jnp.sqrt(whole(amat * amat))

    def step(_, carry):
        yn, zn = carry
        yp, zp = parts(yn), parts(zn)
        tp = parts(1.5 * eye - 0.5 * dot(zp, yp))
        return dot(yp, tp), dot(tp, zp)

    _, zn = lax.fori_loop(0, ITERS, step, (amat / scale, eye))
    zp = parts(zn)
    wbar = jnp.sum(dot(zp, zp) / scale * bs, axis=1, keepdims=True)
    return jnp.sqrt(dof) * zn / jnp.sqrt(scale) + wbar


def cut(units, sizes):
    out = []
    while units:
        out.insert(0, min(units, sizes[min(len(out), len(sizes) - 1)]))
        units -= out[0]
    return out


def plan(piece):
    units = piece // UNIT
    late = max(1, round(units * LATE))
    at, moves = 0, []
    for part in cut(units - late, EARLY_SIZES), cut(late, LATE_SIZES):
        moves.append([])
        for n in part:
            moves[-1].append((at, n))
            at += n
    return units, *moves


def mixed_units(late_moves):
    return late_moves[-2:][0][0]


def tiles(columns):
    n = 1
    while columns % (n * LANES) or columns // n > WIDE:
        n += 1
    return n, columns // n


def mixing(tr):
    members = tr.shape[0]
    wt = tr.T.astype(jnp.bfloat16)
    mean = jnp.full((16, members), 1.0 / members, jnp.bfloat16)
    return jnp.concatenate([wt, mean], axis=0), 1.0 - jnp.sum(wt.astype(jnp.float32), axis=1, keepdims=True)


def mix(lhs, coef, x):
    members = x.shape[0]
    mixed = jnp.dot(lhs, x, preferred_element_type=jnp.float32)
    return (mixed[:members] + coef * mixed[members : members + 1]).astype(x.dtype)


def sum_rounds(nmem, ncol):
    aside = 4 if ncol > 4 else 0
    rounds = [[(b, aside)] for b in bits(nmem)]
    gens = [(0, b) for b in bits(ncol) if b > 1]
    for i in range(0, len(gens), 2):
        pair = gens[i : i + 2]
        if len(pair) == 2:
            pair.append((0, pair[0][1] ^ pair[1][1]))
        rounds.append(pair)
    return rounds


def take(x, index):
    return jnp.take_along_axis(x, jnp.broadcast_to(index, x.shape), axis=1)


def unpack(some, rest, back):
    some, rest = some.astype(jnp.float32), rest.astype(jnp.float32)
    rest = [rest[:, t * LANES : (t + 1) * LANES] for t in range(7)]
    lane = lax.broadcasted_iota(jnp.int32, some.shape, 1)
    last = None
    for t in range(7):
        here = jnp.take_along_axis(rest[t], 112 + lax.rem(lane, 16), axis=1)
        last = here if last is None else jnp.where(lane // 16 == t, here, last)
    blocks = []
    for t, other in enumerate(rest + [last]):
        index = jnp.broadcast_to(back[t : t + 1], some.shape)
        inner = jnp.where(index < LANES, index, index - LANES)
        blocks.append(jnp.where(index < LANES, take(some, inner), take(other, inner)))
    return jnp.concatenate(blocks, axis=1).astype(jnp.bfloat16)


def exchange_kernel(
    nmem, ncol, sa, sb, idx_hbm, val_hbm, wgt_hbm, cnt_hbm, oa, ob, tr, some_out, rest_out, back_out,
    idx, val, wgt, cnt, table_sem, stage, idx_f, val_f, wgt_f, idx_tx, idx_in,
    from_s, from_c, at_s, back, tx, rest_tx, ahead_in, rest_in, hx, cur, got, res, lhs,
    own_sem, stage_sem, idx_s, idx_r, hx_s, hx_r, st_s, st_r, red_s, red_r, pair_s, pair_r, known,
):
    me = lax.axis_index("mem")
    col = lax.axis_index("col")
    mk = sa.shape[0]
    members = mk * nmem
    piece = sa.shape[1] // nmem
    nblk = idx.shape[2]
    units, early_moves, late_moves = plan(piece)
    early = late_moves[0][0]
    late = units - early
    state, out = (sa, sb), (oa, ob)
    peers = [lax.rem(me + d, nmem) for d in range(1, nmem)]
    rounds = sum_rounds(nmem, ncol)
    greeted = sorted({p for r in rounds for p in r if p[1]})
    paired = ncol > 1
    mate = {"col": col ^ 1}
    hub = lax.rem(col, 2) == 0

    def partner(p):
        return {"mem": me ^ p[0], "col": col ^ p[1]}

    def cols_of(owner, unit, size):
        return pl.ds(pl.multiple_of(owner * piece + unit * UNIT, LANES), size * UNIT)

    my_rows = pl.ds(pl.multiple_of(me * mk, mk), mk)

    loads = []
    for d, p in enumerate(peers):
        for g in range(2):
            loads.append(
                pltpu.make_async_copy(
                    state[g].at[:, cols_of(p, early, late)], stage.at[d, g], stage_sem.at[d, g]
                )
            )
    own = []
    for g in range(2):
        own.append(
            pltpu.make_async_copy(
                state[g].at[:, cols_of(me, 0, units)], out[g].at[my_rows, :], own_sem.at[g]
            )
        )
    tables = []
    for n, (a, b) in enumerate(((idx_hbm, idx), (val_hbm, val), (wgt_hbm, wgt), (cnt_hbm, cnt))):
        tables.append(pltpu.make_async_copy(a, b, table_sem.at[n]))

    barrier = pltpu.get_barrier_semaphore()
    for p in peers:
        pl.semaphore_signal(barrier, inc=1, device_id={"mem": p}, device_id_type=MESH)
    for c in tables:
        c.start()
    @pl.when(hub)
    def _():
        for p in greeted:
            pl.semaphore_signal(barrier, inc=1, device_id=partner(p), device_id_type=MESH)
        pl.semaphore_wait(barrier, len(peers) + len(greeted) + paired)
        if paired:
            pl.semaphore_signal(known, inc=1, device_id=mate, device_id_type=MESH)

    @pl.when(jnp.logical_not(hub))
    def _():
        pl.semaphore_signal(barrier, inc=1, device_id=mate, device_id_type=MESH)
        pl.semaphore_wait(barrier, len(peers))

    each = [(g, d) for g in range(2) for d in range(nmem - 1)]
    moves = []
    for at, size in early_moves + late_moves:
        moves.append([])
        for g, d in each:
            slot = (len(moves) - 1) * len(each) + len(moves[-1])
            if at < early:
                source = state[g].at[:, cols_of(peers[d], at, size)]
                target = out[g].at[my_rows, pl.ds(at * UNIT, size * UNIT)]
            else:
                where = pl.ds((at - early) * REST, size * REST)
                source, target = rest_tx.at[d, g, :, where], rest_in.at[me, g, :, where]
                if (at, size) == late_moves[-1]:
                    target = rest_out.at[me, g]
            moves[-1].append(
                pltpu.make_async_remote_copy(
                    source, target, st_s.at[slot], st_r.at[slot],
                    device_id={"mem": peers[d]}, device_id_type=MESH,
                )
            )
    first = len([at for at, _ in early_moves if 0 < at < FIRST]) + 1

    def start(some):
        for ms in some:
            for m in ms:
                m.start()

    start(moves[:1])
    for c in loads + own:
        c.start()

    for c in tables:
        c.wait()
    slot_of = lax.broadcasted_iota(jnp.int32, (16, nblk), 0)
    diag = (
        lax.broadcasted_iota(jnp.int32, (8, LANES), 0)
        == lax.broadcasted_iota(jnp.int32, (8, LANES), 1) // 16
    )

    def flat(x):
        x = jnp.concatenate([x] * 8, axis=0).T.reshape(units, 8, LANES)
        return jnp.sum(jnp.where(diag[None], x, 0.0), axis=1)

    for g in range(2):
        rows = flat(idx[g].astype(jnp.float32))
        idx_f[g] = rows.astype(jnp.int32)
        idx_tx[g] = rows[early:].astype(jnp.bfloat16)
    for g in range(2):
        live = slot_of < cnt[g : g + 1, :]
        wgt_f[g] = flat(jnp.where(live, wgt[g], 0.0))
        val_f[g] = flat(val[g])

    idx_copies = []
    for d, p in enumerate(peers):
        idx_copies.append(
            pltpu.make_async_remote_copy(
                idx_tx, idx_in.at[d], idx_s.at[d], idx_r.at[d], device_id={"mem": p}, device_id_type=MESH
            )
        )
        idx_copies[-1].start()
    start(moves[1:first])

    def gather(s, index):
        rows = s.shape[0]
        lane = lax.broadcasted_iota(jnp.int32, (rows, LANES), 1) // 16
        s = s.astype(jnp.float32)
        index = jnp.broadcast_to(index, (rows, LANES))
        picked = None
        for j in range(8):
            here = jnp.take_along_axis(s[:, j * LANES : (j + 1) * LANES], index, axis=1)
            picked = here if picked is None else jnp.where(lane == j, here, picked)
        return picked

    def lanes_of(unit):
        return pl.ds(pl.multiple_of(unit * LANES, LANES), LANES)

    def unit_cols(unit):
        return pl.ds(pl.multiple_of(unit * UNIT, LANES), UNIT)

    shape = (late * 8, LANES)
    lane = lax.broadcasted_iota(jnp.int32, shape, 1)
    block = lax.rem(lax.broadcasted_iota(jnp.int32, shape, 0), 8)
    lane_f = lane.astype(jnp.float32)
    upto = (
        lax.broadcasted_iota(jnp.int32, (LANES, LANES), 0)
        <= lax.broadcasted_iota(jnp.int32, (LANES, LANES), 1)
    ).astype(jnp.bfloat16)

    def spread(rows):
        return jnp.broadcast_to(rows[:, None, :], (late, 8, LANES)).reshape(shape)

    def own_slots(x):
        return jnp.sum(jnp.where(block == lane // 16, x, 0.0).reshape(late, 8, LANES), axis=1)

    def ranks(table):
        seen = jnp.zeros(shape, jnp.float32)
        for s in range(16):
            column = jnp.take_along_axis(table, block * 16 + s, axis=1)
            seen = jnp.where(column == lane_f, 1.0, seen)
        before = jnp.dot(seen.astype(jnp.bfloat16), upto, preferred_element_type=jnp.float32)
        spare = 16.0 - before[:, LANES - 1 :]
        other = lane_f + 1.0 - before
        ahead = before + jnp.minimum(other, spare)
        return (seen > 0.0) | (other <= spare), ahead, lane_f + 1.0 - ahead

    def search(rank, limit):
        at = jnp.zeros(shape, jnp.int32)
        for b in (64, 32, 16, 8, 4, 2, 1):
            here = jnp.take_along_axis(rank, at + (b - 1), axis=1)
            at = jnp.where(here <= limit, at + b, at)
        return at

    for g in range(2):
        table = spread(idx_tx[g].astype(jnp.float32))
        goes, ahead, behind = ranks(table)
        place = jnp.where(goes, (16 * block).astype(jnp.float32) + ahead - 1.0, LANES + behind - 1.0)
        back[g] = place.astype(jnp.int32)
        back_out[g] = place[(late_moves[-1][0] - early) * 8 :].astype(jnp.int32)
        slots = own_slots(jnp.take_along_axis(ahead, table.astype(jnp.int32), axis=1))
        first_lane = (lax.broadcasted_iota(jnp.int32, (late, LANES), 1) // 16) * 16
        at_s[g] = slots.astype(jnp.int32) - 1 + first_lane

    for c in loads:
        c.wait()
    for c in idx_copies:
        c.wait()
    tail = lax.broadcasted_iota(jnp.int32, (mk, LANES), 1) >= 112

    def send_to(d, _):
        for g in range(2):
            table = spread(idx_in[nmem - 2 - d, g].astype(jnp.float32))
            _, ahead, behind = ranks(table)
            from_s[g] = own_slots(search(ahead, lax.rem(lane, 16).astype(jnp.float32)).astype(jnp.float32)).astype(jnp.int32)
            source = search(behind, lane_f)
            last = spread(source.astype(jnp.float32).reshape(late, 8, LANES)[:, 7, :])
            last = jnp.take_along_axis(last, jnp.clip(16 * block + lane - 112, 0, LANES - 1), axis=1)
            from_c[g] = jnp.where(lane < 112, source, last.astype(jnp.int32))

        def send_row(u, _):
            for g in range(2):
                x = stage[d, g, :, unit_cols(u)].astype(jnp.float32)
                tx[d, g, :, lanes_of(u)] = gather(x, from_s[g, pl.ds(u, 1), :]).astype(jnp.bfloat16)
                rest = []
                for t in range(7):
                    index = from_c[g, pl.ds(u * 8 + t, 1), :]
                    rest.append(
                        jnp.where(tail, take(x[:, 7 * LANES :], index), take(x[:, t * LANES : (t + 1) * LANES], index))
                    )
                where = pl.ds(pl.multiple_of(u * REST, LANES), REST)
                rest_tx[d, g, :, where] = jnp.concatenate(rest, axis=1).astype(jnp.bfloat16)
            return 0

        lax.fori_loop(0, late, send_row, 0)
        return 0

    lax.fori_loop(0, nmem - 1, send_to, 0)
    hx_copies = []
    for d, p in enumerate(peers):
        hx_copies.append(
            pltpu.make_async_remote_copy(
                tx.at[d], ahead_in.at[me], hx_s.at[d], hx_r.at[d], device_id={"mem": p}, device_id_type=MESH
            )
        )
    for c in own:
        c.wait()
    for g in range(2):

        def own_row(u, _):
            picked = gather(out[g][my_rows, unit_cols(early + u)], idx_f[g, pl.ds(early + u, 1), :])
            hx[me, g, :, lanes_of(u)] = picked.astype(jnp.bfloat16)
            return 0

        lax.fori_loop(0, late, own_row, 0)
    for c in hx_copies:
        c.start()
    start(moves[first:])

    def product(acc, x, value, weight):
        hmean = jnp.sum(x, axis=0, keepdims=True) / members
        rest = jnp.zeros((ROWS - members - 1, x.shape[1]), jnp.float32)
        aug = jnp.concatenate([x - hmean, value - hmean, rest], axis=0)
        return acc + lax.dot_general(
            aug * weight, aug, (((1,), (1,)), ((), ())), precision=HIGH,
            preferred_element_type=jnp.float32,
        )

    def early_sum(u, acc):
        for n, (at, _) in enumerate(early_moves):

            @pl.when(u == at)
            def _():
                for m in moves[n]:
                    m.wait_recv()

        x = [gather(out[g][:, unit_cols(u)], idx_f[g, pl.ds(u, 1), :]) for g in range(2)]
        value = [val_f[g, pl.ds(u, 1), :] for g in range(2)]
        weight = [wgt_f[g, pl.ds(u, 1), :] for g in range(2)]
        return product(acc, *(jnp.concatenate(t, axis=1) for t in (x, value, weight)))

    acc = lax.fori_loop(0, early - 1, early_sum, jnp.zeros((ROWS, ROWS), jnp.float32))
    for c in hx_copies:
        c.wait()

    def arrange(n, _):
        p = lax.rem(me + 1 + n // late, nmem)
        u = lax.rem(n, late)
        for g in range(2):
            x = ahead_in[p, g, :, lanes_of(u)].astype(jnp.float32)
            hx[p, g, :, lanes_of(u)] = take(x, at_s[g, pl.ds(u, 1), :]).astype(jnp.bfloat16)
        return 0

    lax.fori_loop(0, (nmem - 1) * late, arrange, 0)
    some_out[...] = ahead_in[:, :, :, (late_moves[-1][0] - early) * LANES :]

    def late_sum(u, acc):
        x, value, weight = [], [], []
        for g in range(2):
            x.append(
                jnp.concatenate([hx[m, g, :, lanes_of(u)].astype(jnp.float32) for m in range(nmem)], axis=0)
            )
            value.append(val_f[g, pl.ds(early + u, 1), :])
            weight.append(wgt_f[g, pl.ds(early + u, 1), :])
        return product(acc, *(jnp.concatenate(t, axis=1) for t in (x, value, weight)))

    acc = lax.fori_loop(0, late, late_sum, acc)
    acc = early_sum(early - 1, acc)

    live = cnt[...].astype(jnp.float32)
    live = jnp.sum(jnp.sum(live, axis=1, keepdims=True), axis=0, keepdims=True)
    acc = pack(acc, live, members)

    def to_mate(n, src, dst):
        return pltpu.make_async_remote_copy(
            src, dst, pair_s.at[n], pair_r.at[n], device_id=mate, device_id_type=MESH
        )

    @pl.when(hub)
    def _():
        total = acc
        if paired:
            to_mate(0, res, got.at[0]).wait_recv()
            total = total + got[0]
        slot = 1
        for n, r in enumerate(rounds):
            cur[n] = total
            copies = []
            for p in r:
                copies.append(
                    pltpu.make_async_remote_copy(
                        cur.at[n], got.at[slot + len(copies)],
                        red_s.at[slot + len(copies)], red_r.at[slot + len(copies)],
                        device_id=partner(p), device_id_type=MESH,
                    )
                )
            for c in copies:
                c.start()
            for c in copies:
                c.wait()
            total = total + got[slot]
            if len(r) == 3:
                total = total + (got[slot + 1] + got[slot + 2])
            slot += len(r)
        res[...] = total
        if paired:
            to_mate(1, res, res).start()

    @pl.when(jnp.logical_not(hub))
    def _():
        cur[0] = acc
        pl.semaphore_wait(known, 1)
        send = to_mate(0, cur.at[0], got.at[0])
        send.start()
        send.wait_send()
        to_mate(1, res, res).wait_recv()

    weights = transform_of(res[...], members)
    tr[...] = weights
    left, coef = mixing(weights)
    lhs[...] = left
    count, width = tiles(early * UNIT)

    def mix_tile(i, _):
        where = pl.ds(pl.multiple_of(i * width, LANES), width)
        for g in range(2):
            out[g][:, where] = mix(lhs[...], coef, out[g][:, where])
        return 0

    lax.fori_loop(0, count, mix_tile, 0)

    def put_back(n, _):
        p = lax.rem(me + 1 + lax.rem(n, nmem - 1), nmem)
        u = n // (nmem - 1)
        rows = pl.ds(pl.multiple_of(p * mk, mk), mk)
        for g in range(2):
            out[g][rows, unit_cols(early + u)] = unpack(
                ahead_in[p, g, :, lanes_of(u)],
                rest_in[p, g, :, pl.ds(pl.multiple_of(u * REST, LANES), REST)],
                back[g, pl.ds(pl.multiple_of(u * 8, 8), 8), :],
            )
        return 0

    for (at, size), ms in zip(late_moves, moves[len(early_moves) :]):
        for m in ms:
            m.wait_recv()
        if (at, size) != late_moves[-1]:
            begin = (at - early) * (nmem - 1)
            lax.fori_loop(begin, begin + size * (nmem - 1), put_back, 0)
        if at < mixed_units(late_moves):
            where = pl.ds(at * UNIT, size * UNIT)
            for g in range(2):
                out[g][:, where] = mix(lhs[...], coef, out[g][:, where])
    for ms in moves:
        for m in ms:
            m.wait_send()

    @pl.when(hub)
    def _():
        if paired:
            to_mate(1, res, res).wait_send()


def exchange(state_a, state_b, idx, val, wgt, cnt):
    nmem, ncol = lax.axis_size("mem"), lax.axis_size("col")
    mk, held = state_a.shape
    piece = held // nmem
    members = mk * nmem
    units, early_moves, late_moves = plan(piece)
    late = units - late_moves[0][0]
    rounds = sum_rounds(nmem, ncol)
    slots = 1 + sum(len(r) for r in rounds)
    moves = 2 * (nmem - 1) * len(early_moves + late_moves)
    used = members * members // LANES + 8
    dma = pltpu.SemaphoreType.DMA
    hbm = pl.BlockSpec(memory_space=pltpu.HBM)
    vmem = pl.BlockSpec(memory_space=pltpu.VMEM)
    return pl.pallas_call(
        functools.partial(exchange_kernel, nmem, ncol),
        out_shape=(
            pltpu.VMEM((members, piece), jnp.bfloat16),
            pltpu.VMEM((members, piece), jnp.bfloat16),
            pltpu.VMEM((members, members), jnp.float32),
            pltpu.VMEM((nmem, 2, mk, late_moves[-1][1] * LANES), jnp.bfloat16),
            pltpu.VMEM((nmem, 2, mk, late_moves[-1][1] * REST), jnp.bfloat16),
            pltpu.VMEM((2, late_moves[-1][1] * 8, LANES), jnp.int32),
        ),
        in_specs=[hbm] * 6,
        out_specs=(vmem,) * 6,
        scratch_shapes=[
            *(pltpu.VMEM(x.shape, x.dtype) for x in (idx, val, wgt, cnt)),
            dma((4,)),
            pltpu.VMEM((nmem - 1, 2, mk, late * UNIT), jnp.bfloat16),
            pltpu.VMEM((2, units, LANES), jnp.int32),
            pltpu.VMEM((2, units, LANES), jnp.float32),
            pltpu.VMEM((2, units, LANES), jnp.float32),
            pltpu.VMEM((2, late, LANES), jnp.bfloat16),
            pltpu.VMEM((nmem - 1, 2, late, LANES), jnp.bfloat16),
            pltpu.VMEM((2, late, LANES), jnp.int32),
            pltpu.VMEM((2, late * 8, LANES), jnp.int32),
            pltpu.VMEM((2, late, LANES), jnp.int32),
            pltpu.VMEM((2, late * 8, LANES), jnp.int32),
            pltpu.VMEM((nmem - 1, 2, mk, late * LANES), jnp.bfloat16),
            pltpu.VMEM((nmem - 1, 2, mk, late * REST), jnp.bfloat16),
            pltpu.VMEM((nmem, 2, mk, late * LANES), jnp.bfloat16),
            pltpu.VMEM((nmem, 2, mk, late * REST), jnp.bfloat16),
            pltpu.VMEM((nmem, 2, mk, late * LANES), jnp.bfloat16),
            pltpu.VMEM((max(1, len(rounds)), used, LANES), jnp.float32),
            pltpu.VMEM((slots, used, LANES), jnp.float32),
            pltpu.VMEM((used, LANES), jnp.float32),
            pltpu.VMEM((members + 16, members), jnp.bfloat16),
            dma((2,)),
            dma((nmem - 1, 2)),
            dma((nmem - 1,)),
            dma((nmem - 1,)),
            dma((nmem - 1,)),
            dma((nmem - 1,)),
            dma((moves,)),
            dma((moves,)),
            dma((slots,)),
            dma((slots,)),
            dma((2,)),
            dma((2,)),
            pltpu.SemaphoreType.REGULAR,
        ],
        compiler_params=pltpu.CompilerParams(
            collective_id=0, has_side_effects=True, vmem_limit_bytes=40 * 2**20
        ),
        name="exchange",
    )(*(pltpu.with_memory_space_constraint(x, pltpu.HBM) for x in (state_a, state_b, idx, val, wgt, cnt)))


def write_kernel(nmem, ready, xa, xb, tr, some, rest, back, oa, ob, ot, mid, end, sems, tr_sem):
    me = lax.axis_index("mem")
    mk = xa.shape[0] // nmem
    piece = xa.shape[1]
    last = end.shape[2]
    pairs = list(enumerate(((xa, oa), (xb, ob))))
    copies = [pltpu.make_async_copy(tr, ot, tr_sem)]
    half = ready // PARTS
    for i in range(PARTS):
        for g, (x, o) in pairs:
            where = pl.ds(i * half, half)
            copies.append(pltpu.make_async_copy(x.at[:, where], o.at[:, where], sems.at[g, i]))
    for c in copies:
        c.start()

    def send(g, n, source, target):
        copies.append(pltpu.make_async_copy(source, target, sems.at[g, n]))
        copies[-1].start()

    lhs, coef = mixing(tr[...])
    if ready < piece - last:
        for g, (x, o) in pairs:
            where = pl.ds(ready, piece - last - ready)
            mid[g] = mix(lhs, coef, x[:, where])
            send(g, PARTS, mid.at[g], o.at[:, where])
    for g, (x, o) in pairs:
        where = pl.ds(piece - last, last)
        end[g] = x[:, where]
        for d in range(1, nmem):
            p = lax.rem(me + d, nmem)
            for u in range(last // UNIT):
                end[g, pl.ds(pl.multiple_of(p * mk, mk), mk), u * UNIT : (u + 1) * UNIT] = unpack(
                    some[p, g, :, u * LANES : (u + 1) * LANES],
                    rest[p, g, :, u * REST : (u + 1) * REST],
                    back[g, u * 8 : (u + 1) * 8, :],
                )
        end[g] = mix(lhs, coef, end[g])
        send(g, PARTS + 1, end.at[g], o.at[:, where])
    for c in copies:
        c.wait()


def write(xa, xb, tr, some, rest, back):
    members, piece = xa.shape
    _, _, late_moves = plan(piece)
    ready, last = mixed_units(late_moves) * UNIT, late_moves[-1][1] * UNIT
    vmem = pl.BlockSpec(memory_space=pltpu.VMEM)
    hbm = pl.BlockSpec(memory_space=pltpu.HBM)
    return pl.pallas_call(
        functools.partial(write_kernel, some.shape[0], ready),
        out_shape=tuple(jax.ShapeDtypeStruct(x.shape, x.dtype) for x in (xa, xb, tr)),
        in_specs=[vmem] * 6,
        out_specs=(hbm, hbm, hbm),
        scratch_shapes=[
            pltpu.VMEM((2, members, max(LANES, piece - last - ready)), xa.dtype),
            pltpu.VMEM((2, members, last), xa.dtype),
            pltpu.SemaphoreType.DMA((2, PARTS + 2)),
            pltpu.SemaphoreType.DMA,
        ],
        compiler_params=pltpu.CompilerParams(vmem_limit_bytes=40 * 2**20),
        name="write",
    )(xa, xb, tr, some, rest, back)


def shards(state_a, state_b, obs_index, observation_count, obs_value, obs_weight):
    tables = [jnp.transpose(x, (0, 2, 1)) for x in (obs_index, obs_value, obs_weight)]
    return write(*exchange(state_a, state_b, *tables, observation_count))


def solution(mesh):
    return jax.shard_map(
        shards,
        mesh=mesh,
        in_specs=(
            P("mem", "col"),
            P("mem", "col"),
            P(None, ("col", "mem"), None),
            P(None, ("col", "mem")),
            P(None, ("col", "mem"), None),
            P(None, ("col", "mem"), None),
        ),
        out_specs=(P(None, ("col", "mem")), P(None, ("col", "mem")), P()),
        check_vma=False,
    )
```
